512 devices in a mesh: groups: 2 (over y), inner: 32 (over z), outer: 4 (over x), head: 2 (over core).
Axes of the slice: x: 4, y: 2, z: 32, core: 2. Of those that a mesh axis runs over, the one named last changes fastest.
The devices are a block of a 4x8x32 slice.
Arguments:
- queries: bfloat16 [8, 4096, 8, 128], P(('groups', 'outer'), 'inner', 'head'), parts along dimension 0, may hold values from -112 to 112
- keys: bfloat16 [8, 4096, 128], P(('groups', 'outer'), 'inner'), parts along dimension 0, may hold values from -4 to 4
- values: bfloat16 [8, 4096, 128], P(('groups', 'outer'), 'inner'), parts along dimension 0, may hold values from -6 to 6
- out: bfloat16 [8, 4096, 8, 128], P(('groups', 'outer'), 'inner', 'head'), parts along dimension 0, may hold values from -6 to 6, as said below
- log_total: float32 [8, 8, 4096], P(('groups', 'outer'), 'head', 'inner'), parts along dimension 0, as said below
- d_out: bfloat16 [8, 4096, 8, 128], P(('groups', 'outer'), 'inner', 'head'), parts along dimension 0, may hold values from -6 to 6
- span_order: int32 [8, 64], P(('groups', 'outer')), parts along dimension 0, may hold values from 0 to 63, as said below
Outputs:
- grad_queries: bfloat16 [8, 4096, 8, 128], P(('groups', 'outer'), 'inner', 'head'), parts along dimension 0
- grad_keys: bfloat16 [8, 4096, 128], P(('groups', 'outer'), 'inner'), parts along dimension 0
- grad_values: bfloat16 [8, 4096, 128], P(('groups', 'outer'), 'inner'), parts along dimension 0
The draws below stay inside these ranges and needn't reach their ends.
There are 2 independent parts, one for each index of `groups`. The reference program is written for one: setup_inputs(seed, part) draws one part's arguments, and reference() takes and returns one part's arrays. A program takes and returns all parts, laid end to end along the dimension named above; each array names one. Nothing has to cross between parts.
Inputs may be any that keep to these rules, and one draw needn't show every extreme that they name: `span_order`: each row is a permutation of 0 to 63. `out`: the causal softmax attention output of queries, keys and values in the order given by span_order, rounded to bfloat16. `log_total`: the log of the causal softmax total of each query row and head for the same inputs.
All inputs are finite; a program needn't handle non-finite values.
Results may differ from the reference program's by a relative error of at most 0.0054.
Values may be sent and summed in bfloat16 or wider, within the bound.
No kernel may reach another device: no remote copies, remote signals or barrier semaphores. Data moves between devices by JAX's collectives and lax.ppermute only.
A program may use at most 64 MiB of HBM per device.

```python
import math
import jax
import jax.numpy as jnp
from jax import lax

HD = 128
GROUP_HEADS = 8
SPAN = 64
SEQ = 4096
SPANS = 64
BATCH = 4


def layout_positions_drawn(block_order):
    rows = jnp.arange(SEQ, dtype=jnp.int32)
    tok_rows = 2 * SPAN
    owner = rows // tok_rows
    offset = rows % tok_rows
    span = block_order[(2 * owner + offset // SPAN).astype(jnp.int32)]
    return (span * SPAN + offset % SPAN).astype(jnp.int32)


def order_row(row_key):
    return jax.random.permutation(row_key, SPANS)


def base_draw(key):
    order_keys = jax.random.split(jax.random.fold_in(key, 100), BATCH)
    block_order = jax.vmap(order_row)(order_keys).astype(jnp.int32)
    base_keys = jnp.clip(jax.random.normal(jax.random.fold_in(key, 101), (BATCH, SEQ, HD), jnp.float32), -4.0, 4.0)
    base_queries = jnp.clip(jax.random.normal(jax.random.fold_in(key, 102), (BATCH, SEQ, GROUP_HEADS, HD), jnp.float32), -4.0, 4.0)
    base_values = jnp.clip(jax.random.normal(jax.random.fold_in(key, 106), (BATCH, SEQ, HD), jnp.float32), -6.0, 6.0)
    return (base_queries.astype(jnp.bfloat16), base_keys.astype(jnp.bfloat16), base_values.astype(jnp.bfloat16), block_order)


def forward_draw(key):
    queries, keys, values, block_order = base_draw(key)
    softmax_scale = 1.0 / math.sqrt(HD)
    tok_rows = 2 * SPAN

    def one_sequence(items):
        seq_queries, seq_keys, seq_values, seq_order = items
        positions = layout_positions_drawn(seq_order)
        key_float = seq_keys.astype(jnp.float32)
        value_float = seq_values.astype(jnp.float32)

        def one_block(block_index):
            start = (block_index * tok_rows).astype(jnp.int32)
            query_block = lax.dynamic_slice_in_dim(seq_queries, start, tok_rows, 0).astype(jnp.float32)
            query_pos = lax.dynamic_slice_in_dim(positions, start, tok_rows, 0)
            visible = positions[None, :] <= query_pos[:, None]
            scores = jnp.einsum('thd,ud->htu', query_block, key_float) * softmax_scale
            scores = jnp.where(visible[None], scores, -jnp.inf)
            row_max = jnp.max(scores, axis=-1, keepdims=True)
            block_total = row_max + jnp.log(jnp.sum(jnp.exp(scores - row_max), axis=-1, keepdims=True))
            probs = jnp.exp(scores - block_total)
            block_out = jnp.einsum('htu,ud->thd', probs, value_float)
            return (block_out, block_total[:, :, 0])
        outs, totals = lax.map(one_block, jnp.arange(SEQ // tok_rows, dtype=jnp.int32))
        seq_out = outs.reshape(SEQ, GROUP_HEADS, HD).astype(jnp.bfloat16)
        seq_total = jnp.transpose(totals, (1, 0, 2)).reshape(GROUP_HEADS, SEQ)
        return (seq_out, seq_total)
    return lax.map(one_sequence, (queries, keys, values, block_order))


def draw_queries(key, part):
    return base_draw(key)[0]


def draw_keys(key, part):
    return base_draw(key)[1]


def draw_values(key, part):
    return base_draw(key)[2]


def draw_span_order(key, part):
    return base_draw(key)[3]


def draw_out(key, part):
    return forward_draw(key)[0]


def draw_log_total(key, part):
    return forward_draw(key)[1].astype(jnp.float32)


def block_levels(rng, dims, shards, least, largest):
    factor_of = 1.0
    for position, blocks in shards:
        draws = jax.random.uniform(jax.random.fold_in(jax.random.fold_in(rng, 6), position), (blocks,), jnp.float32, least / len(shards), largest / len(shards))
        factor_of = factor_of * jnp.repeat(jnp.exp(draws), dims[position] // blocks).reshape((-1,) + (1,) * (len(dims) - 1 - position))
    return factor_of


def noise(rng, extent, deviation, reach, shards=(), kind=jnp.bfloat16):
    gain = block_levels(rng, extent, shards, -0.22, 0.18) if shards else 1.0
    values = jax.random.normal(rng, extent, jnp.float32) * deviation * gain
    return jnp.minimum(jnp.maximum(values, -reach), reach).astype(kind)


def setup_inputs(seed: int = 0, part: int = 0) -> dict:
    splits = jax.random.split(jax.random.key(seed), 8)
    part_splits = jax.random.split(jax.random.fold_in(splits[7], part), 8)
    return {
        "queries": draw_queries(jax.random.fold_in(jax.random.fold_in(splits[7], part), 71), part),
        "keys": draw_keys(jax.random.fold_in(jax.random.fold_in(splits[7], part), 71), part),
        "values": draw_values(jax.random.fold_in(jax.random.fold_in(splits[7], part), 71), part),
        "out": draw_out(jax.random.fold_in(jax.random.fold_in(splits[7], part), 71), part),
        "log_total": draw_log_total(jax.random.fold_in(jax.random.fold_in(splits[7], part), 71), part),
        "d_out": noise(part_splits[5], (BATCH, SEQ, GROUP_HEADS, HD), 1.0, 6.0, ((0, 4), (1, 32), (2, 2))),
        "span_order": draw_span_order(jax.random.fold_in(jax.random.fold_in(splits[7], part), 71), part),
    }


def layout_positions(block_order):
    rows = jnp.arange(SEQ, dtype=jnp.int32)
    tok_rows = 2 * SPAN
    owner = rows // tok_rows
    offset = rows % tok_rows
    span = block_order[(2 * owner + offset // SPAN).astype(jnp.int32)]
    return (span * SPAN + offset % SPAN).astype(jnp.int32)

def reference(queries, keys, values, out, log_total, d_out, span_order):
    softmax_scale = 1.0 / math.sqrt(HD)
    tok_rows = 2 * SPAN

    def one_sequence(items):
        seq_queries, seq_keys, seq_values, seq_out, seq_total, seq_grad, seq_order = items
        positions = layout_positions(seq_order)
        key_float = seq_keys.astype(jnp.float32)
        value_float = seq_values.astype(jnp.float32)

        def block(carry, block_index):
            key_total, value_total = carry
            start = (block_index * tok_rows).astype(jnp.int32)
            query_block = lax.dynamic_slice_in_dim(seq_queries, start, tok_rows, 0).astype(jnp.float32)
            grad_block = lax.dynamic_slice_in_dim(seq_grad, start, tok_rows, 0).astype(jnp.float32)
            out_block = lax.dynamic_slice_in_dim(seq_out, start, tok_rows, 0).astype(jnp.float32)
            total_block = lax.dynamic_slice_in_dim(seq_total, start, tok_rows, 1)
            query_pos = lax.dynamic_slice_in_dim(positions, start, tok_rows, 0)
            visible = positions[None, :] <= query_pos[:, None]
            scores = jnp.einsum('thd,ud->htu', query_block, key_float) * softmax_scale
            probs = jnp.exp(jnp.where(visible[None], scores - total_block[:, :, None], -jnp.inf))
            grad_probs = jnp.einsum('thd,ud->htu', grad_block, value_float)
            row_delta = jnp.transpose(lax.optimization_barrier(jnp.sum(out_block * grad_block, axis=-1)))[:, :, None]
            grad_scores = probs * (grad_probs - row_delta) * softmax_scale
            scores_half = lax.optimization_barrier(grad_scores.astype(jnp.bfloat16)).astype(jnp.float32)
            probs_half = lax.optimization_barrier(probs.astype(jnp.bfloat16)).astype(jnp.float32)
            query_grad = jnp.einsum('htu,ud->thd', scores_half, key_float).astype(jnp.bfloat16)
            key_total = key_total + jnp.einsum('htu,thd->ud', scores_half, query_block)
            value_total = value_total + jnp.einsum('htu,thd->ud', probs_half, grad_block)
            return ((key_total, value_total), query_grad)
        zeros = jnp.zeros((SEQ, HD), jnp.float32)
        (key_total, value_total), query_grads = lax.scan(block, (zeros, zeros), jnp.arange(SEQ // tok_rows, dtype=jnp.int32))
        grad_queries = query_grads.reshape(SEQ, GROUP_HEADS, HD)
        return (grad_queries, key_total.astype(jnp.bfloat16), value_total.astype(jnp.bfloat16))
    return lax.map(one_sequence, (queries, keys, values, out, log_total, d_out, span_order))
```

```python
import math

import jax
import jax.numpy as jnp
from jax import lax
from jax.experimental import pallas as pl
from jax.experimental.pallas import tpu as pltpu
from jax.sharding import PartitionSpec as P

LOG2E = math.log2(math.e)
NEAR = 4


def near_groups(size):
    return [[base + i for i in range(NEAR)] for base in range(0, size, NEAR)]


def far_groups(size):
    return [list(range(first, size, NEAR)) for first in range(NEAR)]


def kernel(scale, tile, spans, own_spans, kv, qa, qb, da, db, stat_a, stat_b, dqa, dqb, dkv, acc):
    width = qa.shape[1]
    heads, toks = stat_a.shape[1], stat_a.shape[2]
    span_rows = toks // 2
    tiles = kv.shape[0] // tile
    per_tile = tile // span_rows
    token = lax.broadcasted_iota(jnp.int32, (tile, toks), 1)
    row = lax.broadcasted_iota(jnp.int32, (tile, toks), 0)
    query_span = jnp.where(token < span_rows, own_spans[0], own_spans[1])
    query_pos = query_span * span_rows + token % span_rows
    row_in_span = row % span_rows
    row_span = row // span_rows
    acc[...] = jnp.zeros_like(acc)

    def step(index, carry):
        start = pl.multiple_of(index * tile, tile)
        k = kv[pl.ds(start, tile), :width]
        v = kv[pl.ds(start, tile), width:]
        key_span = jnp.full((tile, toks), spans[index * per_tile], jnp.int32)
        for j in range(1, per_tile):
            key_span = jnp.where(row_span == j, spans[index * per_tile + j], key_span)
        visible = key_span * span_rows + row_in_span <= query_pos
        dk = jnp.zeros((tile, width), jnp.float32)
        dv = jnp.zeros((tile, width), jnp.float32)
        for half, (q_ref, d_ref, stat) in enumerate(((qa, da, stat_a), (qb, db, stat_b))):
            q = q_ref[...]
            d = d_ref[...]
            nt = (((1,), (1,)), ((), ()))
            s = lax.dot_general(k, q, nt, preferred_element_type=jnp.float32)
            g = lax.dot_general(v, d, nt, preferred_element_type=jnp.float32)
            probs, grads = [], []
            for h in range(heads):
                cols = slice(h * toks, (h + 1) * toks)
                p = jnp.exp2(s[:, cols] * (scale * LOG2E) - stat[0, h : h + 1, :])
                p = jnp.where(visible, p, 0.0)
                probs.append(p.astype(jnp.bfloat16))
                grads.append((p * (g[:, cols] - stat[1, h : h + 1, :])).astype(jnp.bfloat16))
            p = jnp.concatenate(probs, axis=1)
            ds = jnp.concatenate(grads, axis=1)
            dv = dv + jnp.dot(p, d, preferred_element_type=jnp.float32)
            dk = dk + jnp.dot(ds, q, preferred_element_type=jnp.float32)
            acc[half] += lax.dot_general(
                ds, k, (((0,), (0,)), ((), ())), preferred_element_type=jnp.float32
            )
        dkv[pl.ds(start, tile), :width] = (dk * scale).astype(jnp.bfloat16)
        dkv[pl.ds(start, tile), width:] = dv.astype(jnp.bfloat16)
        return carry

    lax.fori_loop(0, tiles, step, 0)
    dqa[...] = acc[0] * scale
    dqb[...] = (acc[1] * scale).astype(jnp.bfloat16)


def attention_grads(spans, own_spans, kv, qa, qb, da, db, stat_a, stat_b):
    rows, width = qa.shape
    keys = kv.shape[0]
    tile = min(256, keys)
    smem = pl.BlockSpec(memory_space=pltpu.SMEM)
    vmem = pl.BlockSpec(memory_space=pltpu.VMEM)

    def body(*refs):
        kernel(1.0 / math.sqrt(width), tile, *refs)

    return pl.pallas_call(
        body,
        out_shape=(
            jax.ShapeDtypeStruct((rows, width), jnp.float32),
            jax.ShapeDtypeStruct((rows, width), jnp.bfloat16),
            jax.ShapeDtypeStruct((keys, 2 * width), jnp.bfloat16),
        ),
        in_specs=[smem, smem] + [vmem] * 7,
        out_specs=(vmem, vmem, vmem),
        scratch_shapes=[pltpu.VMEM((2, rows, width), jnp.float32)],
        compiler_params=pltpu.CompilerParams(vmem_limit_bytes=32 * 1024 * 1024),
        cost_estimate=pl.CostEstimate(
            flops=2 * 5 * 2 * rows * keys * width,
            bytes_accessed=4 * keys * width * 2,
            transcendentals=2 * rows * keys,
        ),
    )(spans, own_spans, kv, qa, qb, da, db, stat_a, stat_b)


def body(queries, keys, values, out, log_total, d_out, span_order):
    size = lax.axis_size("inner")
    place = lax.axis_index("inner")
    core = lax.axis_index("head")
    toks, heads, width = queries.shape[1:]
    half = toks // 2
    far = size // NEAR
    swap = [(0, 1), (1, 0)]

    qa = jnp.transpose(queries[0], (1, 0, 2)).reshape(heads * toks, width)
    da = jnp.transpose(d_out[0], (1, 0, 2)).reshape(heads * toks, width)
    delta = jnp.transpose(
        jnp.sum(out[0].astype(jnp.float32) * d_out[0].astype(jnp.float32), axis=-1)
    )
    stat_a = jnp.stack([log_total[0] * LOG2E, delta])
    qda = jnp.concatenate([qa, da])
    qdb = lax.ppermute(qda, "head", swap)
    stat_b = lax.ppermute(stat_a, "head", swap)
    qb, db = qdb[: heads * toks], qdb[heads * toks :]

    kv = jnp.concatenate([keys[0], values[0]], axis=1)
    kv = lax.dynamic_slice_in_dim(kv, core * half, half, 0)
    kv = lax.all_gather(kv, "inner", axis_index_groups=far_groups(size), tiled=True)
    kv = jnp.broadcast_to(kv[None], (NEAR, *kv.shape)).reshape(NEAR * far * half, 2 * width)
    kv = lax.all_to_all(kv, "inner", 0, 0, axis_index_groups=near_groups(size), tiled=True)

    order = span_order[0].reshape(far, NEAR, 2)
    spans = jnp.where(core == 0, order[:, :, 0], order[:, :, 1]).T.reshape(-1)
    own_spans = lax.dynamic_slice_in_dim(span_order[0], 2 * place, 2, 0)
    dqa, dqb, dkv = attention_grads(spans, own_spans, kv, qa, qb, da, db, stat_a, stat_b)

    dq_other = lax.ppermute(dqb, "head", swap)
    dkv = lax.all_to_all(dkv, "inner", 0, 0, axis_index_groups=near_groups(size), tiled=True)
    dkv = jnp.sum(dkv.reshape(NEAR, far * half, 2 * width).astype(jnp.float32), axis=0)
    dkv = dkv.astype(jnp.bfloat16)
    dkv = lax.all_to_all(dkv, "inner", 0, 0, axis_index_groups=far_groups(size), tiled=True)
    dkv = jnp.sum(dkv.reshape(far, half, 2 * width).astype(jnp.float32), axis=0)
    dkv = dkv.astype(jnp.bfloat16)
    other = lax.ppermute(dkv, "head", swap)
    first = jnp.where(core == 0, dkv, other)
    second = jnp.where(core == 0, other, dkv)
    dkv = jnp.concatenate([first, second])

    dq = (dqa + dq_other.astype(jnp.float32)).astype(jnp.bfloat16)
    dq = jnp.transpose(dq.reshape(heads, toks, width), (1, 0, 2))
    return dq[None], dkv[None, :, :width], dkv[None, :, width:]


def solution(mesh):
    in_specs = (
        P(("groups", "outer"), "inner", "head", None),
        P(("groups", "outer"), "inner", None),
        P(("groups", "outer"), "inner", None),
        P(("groups", "outer"), "inner", "head", None),
        P(("groups", "outer"), "head", "inner"),
        P(("groups", "outer"), "inner", "head", None),
        P(("groups", "outer"), None),
    )
    out_specs = (
        P(("groups", "outer"), "inner", "head", None),
        P(("groups", "outer"), "inner", None),
        P(("groups", "outer"), "inner", None),
    )
    return jax.shard_map(body, mesh=mesh, in_specs=in_specs, out_specs=out_specs, check_vma=False)
```

```python
import functools
import math

import jax
import jax.numpy as jnp
from jax import lax
from jax.experimental import pallas as pl
from jax.experimental.pallas import tpu as pltpu
from jax.sharding import PartitionSpec as P


LOG2E = math.log2(math.e)
PAIR = 2
CALLS = (1, 3, 4)
STAT_ROWS = 16


def split_stats(stats):
    high = lax.reduce_precision(stats, 8, 7)
    middle = lax.reduce_precision(stats - high, 8, 7)
    low = stats - high - middle
    pad = ((0, STAT_ROWS - stats.shape[0]), (0, 0))
    return [jnp.pad(a, pad).astype(jnp.bfloat16) for a in (high, middle, low)]


def kernel(first, count, heads, toks, order, where, kv_a, kv_b, *refs):
    fresh = first == 0
    payloads = refs[:4]
    dq, dkv = refs[4 if fresh else 5 :]
    rows = heads * toks
    span_rows = toks // 2
    ring = kv_a.shape[0]
    width = kv_a.shape[2] // 2
    scale = 1.0 / math.sqrt(width)
    place, core = where[0], where[1]
    step, parity = place // PAIR, place % PAIR
    token = lax.broadcasted_iota(jnp.int32, (toks, toks), 1)
    row = lax.broadcasted_iota(jnp.int32, (toks, toks), 0)
    key_row, token_row = row % span_rows, token % span_rows

    def query_pos(chip):
        span = jnp.where(token < span_rows, order[2 * chip], order[2 * chip + 1])
        return span * span_rows + token_row

    own_pos = query_pos(place)
    near_pos = query_pos(place + 1 - 2 * parity)
    nt = (((1,), (1,)), ((), ()))
    tn = (((0,), (0,)), ((), ()))
    if fresh:
        dq[...] = jnp.zeros_like(dq)
    else:
        dq[...] = refs[4][...]

    def one_block(index, carry):
        turn = first + index
        ahead = jnp.where(core == 0, turn - (ring // 2 - 1), ring // 2 - turn)
        block = lax.rem(step + ahead + ring, ring)
        chip = block * PAIR + parity
        a, b = kv_a[block], kv_b[block]
        kv = jnp.concatenate([jnp.where(core == 0, a, b), jnp.where(core == 0, b, a)])
        k, v = kv[:, :width], kv[:, width:]
        key_span = jnp.where(row < span_rows, order[2 * chip], order[2 * chip + 1])
        key_pos = key_span * span_rows + key_row
        dk = jnp.zeros((toks, width), jnp.float32)
        dv = jnp.zeros((toks, width), jnp.float32)
        for part, payload in enumerate(payloads):
            visible = key_pos <= (own_pos if part < 2 else near_pos)
            q = payload[:rows]
            d = payload[rows : 2 * rows]
            stats = [
                payload[2 * rows + i * STAT_ROWS : 2 * rows + (i + 1) * STAT_ROWS].astype(jnp.float32)
                for i in range(3)
            ]
            stat = stats[0] + stats[1] + stats[2]
            s = lax.dot_general(k, q, nt, preferred_element_type=jnp.float32)
            g = lax.dot_general(v, d, nt, preferred_element_type=jnp.float32)
            probs, grads = [], []
            for h in range(heads):
                cols = slice(h * toks, (h + 1) * toks)
                p = jnp.exp2(s[:, cols] * (scale * LOG2E) - stat[h : h + 1])
                p = jnp.where(visible, p, 0.0)
                probs.append(p.astype(jnp.bfloat16))
                ds = p * (g[:, cols] - stat[heads + h : heads + h + 1]) * scale
                grads.append(ds.astype(jnp.bfloat16))
            p = jnp.concatenate(probs, axis=1)
            ds = jnp.concatenate(grads, axis=1)
            dv = dv + jnp.dot(p, d, preferred_element_type=jnp.float32)
            dk = dk + jnp.dot(ds, q, preferred_element_type=jnp.float32)
            dq[part] += lax.dot_general(ds, k, tn, preferred_element_type=jnp.float32)
        dkv[index, :, :width] = dk
        dkv[index, :, width:] = dv
        return carry

    lax.fori_loop(0, count, one_block, 0)


def attention_grads(first, count, heads, toks, order, where, kv_a, kv_b, payloads, dq):
    width = kv_a.shape[2] // 2
    rows = heads * toks
    smem = pl.BlockSpec(memory_space=pltpu.SMEM)
    vmem = pl.BlockSpec(memory_space=pltpu.VMEM)
    operands = [order, where, kv_a, kv_b, *payloads] + ([] if dq is None else [dq])
    return pl.pallas_call(
        functools.partial(kernel, first, count, heads, toks),
        out_shape=(
            jax.ShapeDtypeStruct((4, rows, width), jnp.float32),
            jax.ShapeDtypeStruct((count, toks, 2 * width), jnp.float32),
        ),
        in_specs=[smem, smem] + [vmem] * (len(operands) - 2),
        out_specs=(vmem, vmem),
        input_output_aliases={} if dq is None else {len(operands) - 1: 0},
        compiler_params=pltpu.CompilerParams(vmem_limit_bytes=16 * 1024 * 1024),
        cost_estimate=pl.CostEstimate(
            flops=2 * 5 * 4 * rows * count * toks * width,
            bytes_accessed=8 * rows * width * 4,
            transcendentals=4 * rows * count * toks,
        ),
    )(*operands)


def body(queries, keys, values, out, log_total, d_out, span_order):
    size = lax.axis_size("inner")
    place = lax.axis_index("inner")
    core = lax.axis_index("head")
    toks, heads, width = queries.shape[1:]
    half = toks // 2
    rows = heads * toks
    both = ("inner", "head")

    def move(array, target):
        pairs = []
        for z in range(size):
            for c in range(2):
                to = target(z, c)
                if to is not None:
                    pairs.append((2 * z + c, 2 * (to[0] % size) + to[1]))
        return lax.ppermute(array, both, pairs)

    partners = (
        lambda z, c: (z, 1 - c),
        lambda z, c: (z ^ 1, c),
        lambda z, c: (z ^ 1, 1 - c),
    )

    delta = jnp.transpose(
        jnp.sum(out[0].astype(jnp.float32) * d_out[0].astype(jnp.float32), axis=-1)
    )
    stats = split_stats(jnp.concatenate([log_total[0] * LOG2E, delta]))
    payload = jnp.concatenate(
        [
            jnp.transpose(queries[0], (1, 0, 2)).reshape(rows, width),
            jnp.transpose(d_out[0], (1, 0, 2)).reshape(rows, width),
            *stats,
        ]
    )
    payloads = [payload]
    for partner in partners:
        payloads.append(move(payload, partner))

    kv = jnp.concatenate([keys[0], values[0]], axis=1)
    kv = lax.dynamic_slice_in_dim(kv, core * half, half, 0)
    groups = [list(range(first, size, PAIR)) for first in range(PAIR)]
    kv_a = lax.all_gather(kv, "inner", axis_index_groups=groups)
    kv_b = move(kv_a, partners[0])

    order = span_order[0]
    where = jnp.stack([place, core]).astype(jnp.int32)
    dq, parts, first = None, [], 0
    for count in CALLS:
        dq, part = attention_grads(
            first, count, heads, toks, order, where, kv_a, kv_b, payloads, dq
        )
        parts += [part[i] for i in range(count)]
        first += count

    total = parts[0].astype(jnp.bfloat16)
    for part in parts[1:]:
        total = move(total, lambda z, c: (z - PAIR, 0) if c == 0 else (z + PAIR, 1))
        total = (total.astype(jnp.float32) + part).astype(jnp.bfloat16)
    one = move(total, lambda z, c: (z, 1) if c == 0 else (z + PAIR, 0))
    two = move(total, lambda z, c: None if c == 0 else (z + PAIR, 1))
    two = jnp.where(core == 0, total, two)
    dkv = (one.astype(jnp.float32) + two.astype(jnp.float32)).astype(jnp.bfloat16)

    query_grad = dq[0]
    for part, partner in enumerate(partners, 1):
        query_grad = query_grad + move(dq[part].astype(jnp.bfloat16), partner).astype(jnp.float32)
    query_grad = query_grad.astype(jnp.bfloat16).reshape(heads, toks, width)
    query_grad = jnp.transpose(query_grad, (1, 0, 2))
    return query_grad[None], dkv[None, :, :width], dkv[None, :, width:]


def solution(mesh):
    in_specs = (
        P(("groups", "outer"), "inner", "head", None),
        P(("groups", "outer"), "inner", None),
        P(("groups", "outer"), "inner", None),
        P(("groups", "outer"), "inner", "head", None),
        P(("groups", "outer"), "head", "inner"),
        P(("groups", "outer"), "inner", "head", None),
        P(("groups", "outer"), None),
    )
    out_specs = (
        P(("groups", "outer"), "inner", "head", None),
        P(("groups", "outer"), "inner", None),
        P(("groups", "outer"), "inner", None),
    )
    return jax.shard_map(
        body, mesh=mesh, in_specs=in_specs, out_specs=out_specs, check_vma=False
    )
```

```python
import functools
import math

import jax
import jax.numpy as jnp
from jax import lax
from jax.experimental import pallas as pl
from jax.experimental.pallas import tpu as pltpu
from jax.sharding import PartitionSpec as P


LOG2E = math.log2(math.e)
NEAR = 4
CALLS = (1, 2, 1)
STAT_ROWS = 16


def split_stats(stats):
    high = lax.reduce_precision(stats, 8, 7)
    middle = lax.reduce_precision(stats - high, 8, 7)
    low = stats - high - middle
    pad = ((0, STAT_ROWS - stats.shape[0]), (0, 0))
    return [jnp.pad(a, pad).astype(jnp.bfloat16) for a in (high, middle, low)]


def kernel(first, count, heads, toks, order, where, mine, theirs, *refs):
    fresh = first == 0
    dq, dkv = refs if fresh else refs[1:]
    rows = heads * toks
    payload = 2 * rows + 3 * STAT_ROWS
    span_rows = toks // 2
    width = mine.shape[1]
    keys = NEAR * payload
    ring = (mine.shape[0] - keys) // toks
    scale = 1.0 / math.sqrt(width)
    place, core = where[0], where[1]
    step, member = place // NEAR, place % NEAR
    token = lax.broadcasted_iota(jnp.int32, (toks, toks), 1)
    row = lax.broadcasted_iota(jnp.int32, (toks, toks), 0)
    key_row, token_row = row % span_rows, token % span_rows
    nt = (((1,), (1,)), ((), ()))
    tn = (((0,), (0,)), ((), ()))
    if fresh:
        dq[...] = jnp.zeros_like(dq)
    else:
        dq[...] = refs[0][...]

    def one_block(index, carry):
        turn = first + index
        ahead = jnp.where(core == 0, turn - (ring // 2 - 1), ring // 2 - turn)
        block = lax.rem(step + ahead + ring, ring)
        chip = block * NEAR + member
        start = pl.multiple_of(keys + block * toks, STAT_ROWS)
        a, b = mine[pl.ds(start, toks)], theirs[pl.ds(start, toks)]
        low, high = jnp.where(core == 0, a, b), jnp.where(core == 0, b, a)
        k = jnp.concatenate([low[:span_rows], high[:span_rows]])
        v = jnp.concatenate([low[span_rows:], high[span_rows:]])
        key_span = jnp.where(row < span_rows, order[2 * chip], order[2 * chip + 1])
        key_pos = key_span * span_rows + key_row
        dk = jnp.zeros((toks, width), jnp.float32)
        dv = jnp.zeros((toks, width), jnp.float32)
        for near in range(NEAR):
            near_chip = step * NEAR + (member ^ near)
            span = jnp.where(token < span_rows, order[2 * near_chip], order[2 * near_chip + 1])
            visible = key_pos <= span * span_rows + token_row
            base = near * payload
            for part, source in ((near, mine), (NEAR + near, theirs)):
                q = source[base : base + rows]
                d = source[base + rows : base + 2 * rows]
                stat = [
                    source[base + 2 * rows + i * STAT_ROWS : base + 2 * rows + (i + 1) * STAT_ROWS]
                    for i in range(3)
                ]
                stat = sum(x.astype(jnp.float32) for x in stat)
                s = lax.dot_general(k, q, nt, preferred_element_type=jnp.float32)
                g = lax.dot_general(v, d, nt, preferred_element_type=jnp.float32)
                probs, grads = [], []
                for h in range(heads):
                    cols = slice(h * toks, (h + 1) * toks)
                    p = jnp.exp2(s[:, cols] * (scale * LOG2E) - stat[h : h + 1])
                    p = jnp.where(visible, p, 0.0)
                    probs.append(p.astype(jnp.bfloat16))
                    ds = p * (g[:, cols] - stat[heads + h : heads + h + 1]) * scale
                    grads.append(ds.astype(jnp.bfloat16))
                p = jnp.concatenate(probs, axis=1)
                ds = jnp.concatenate(grads, axis=1)
                dv = dv + jnp.dot(p, d, preferred_element_type=jnp.float32)
                dk = dk + jnp.dot(ds, q, preferred_element_type=jnp.float32)
                dq[part] += lax.dot_general(ds, k, tn, preferred_element_type=jnp.float32)
        dkv[index, :, :width] = dk
        dkv[index, :, width:] = dv
        return carry

    lax.fori_loop(0, count, one_block, 0)


def attention_grads(first, count, heads, toks, order, where, mine, theirs, dq):
    width = mine.shape[1]
    rows = heads * toks
    smem = pl.BlockSpec(memory_space=pltpu.SMEM)
    vmem = pl.BlockSpec(memory_space=pltpu.VMEM)
    operands = [order, where, mine, theirs] + ([] if dq is None else [dq])
    return pl.pallas_call(
        functools.partial(kernel, first, count, heads, toks),
        out_shape=(
            jax.ShapeDtypeStruct((2 * NEAR, rows, width), jnp.float32),
            jax.ShapeDtypeStruct((count, toks, 2 * width), jnp.float32),
        ),
        in_specs=[smem, smem] + [vmem] * (len(operands) - 2),
        out_specs=(vmem, vmem),
        input_output_aliases={} if dq is None else {len(operands) - 1: 0},
        compiler_params=pltpu.CompilerParams(vmem_limit_bytes=16 * 1024 * 1024),
        cost_estimate=pl.CostEstimate(
            flops=2 * 5 * 2 * NEAR * rows * count * toks * width,
            bytes_accessed=8 * rows * width * 4,
            transcendentals=2 * NEAR * rows * count * toks,
        ),
    )(*operands)


def body(queries, keys, values, out, log_total, d_out, span_order):
    size = lax.axis_size("inner")
    place = lax.axis_index("inner")
    core = lax.axis_index("head")
    toks, heads, width = queries.shape[1:]
    half = toks // 2
    rows = heads * toks

    def move(array, target):
        pairs = []
        for z in range(size):
            for c in range(2):
                to = target(z, c)
                if to is not None:
                    pairs.append((2 * z + c, 2 * (to[0] % size) + to[1]))
        return lax.ppermute(array, ("inner", "head"), pairs)

    def swap(z, c):
        return z, 1 - c

    def near(distance):
        return lambda z, c: (z ^ distance, c)

    delta = jnp.transpose(
        jnp.sum(out[0].astype(jnp.float32) * d_out[0].astype(jnp.float32), axis=-1)
    )
    payload = jnp.concatenate(
        [
            jnp.transpose(queries[0], (1, 0, 2)).reshape(rows, width),
            jnp.transpose(d_out[0], (1, 0, 2)).reshape(rows, width),
            *split_stats(jnp.concatenate([log_total[0] * LOG2E, delta])),
        ]
    )
    payloads = [payload] + [move(payload, near(i)) for i in range(1, NEAR)]

    kv = jnp.concatenate(
        [lax.dynamic_slice_in_dim(a[0], core * half, half, 0) for a in (keys, values)]
    )
    groups = [list(range(first, size, NEAR)) for first in range(NEAR)]
    kv = lax.all_gather(kv, "inner", axis_index_groups=groups, tiled=True)
    mine = jnp.concatenate([*payloads, kv])
    theirs = move(mine, swap)

    order = span_order[0]
    where = jnp.stack([place, core]).astype(jnp.int32)
    dq, parts, first = None, [], 0
    for count in CALLS:
        dq, part = attention_grads(first, count, heads, toks, order, where, mine, theirs, dq)
        parts += [part[i] for i in range(count)]
        first += count

    total = parts[0].astype(jnp.bfloat16)
    for part in parts[1:]:
        total = move(total, lambda z, c: (z - NEAR, 0) if c == 0 else (z + NEAR, 1))
        total = (total.astype(jnp.float32) + part).astype(jnp.bfloat16)
    one = move(total, lambda z, c: (z, 1) if c == 0 else (z + NEAR, 0))
    two = move(total, lambda z, c: None if c == 0 else (z + NEAR, 1))
    two = jnp.where(core == 0, total, two)
    dkv = (one.astype(jnp.float32) + two.astype(jnp.float32)).astype(jnp.bfloat16)

    dq_theirs = move(dq[NEAR:].astype(jnp.bfloat16), swap)
    dq_mine = dq[:NEAR] + dq_theirs.astype(jnp.float32)
    dq_back = [dq_mine[i].astype(jnp.bfloat16) for i in range(1, NEAR)]
    query_grad = dq_mine[0]
    for i in range(1, NEAR):
        back = move(dq_back[i - 1], near(i))
        query_grad = query_grad + back.astype(jnp.float32)
    query_grad = query_grad.astype(jnp.bfloat16).reshape(heads, toks, width)
    query_grad = jnp.transpose(query_grad, (1, 0, 2))
    return query_grad[None], dkv[None, :, :width], dkv[None, :, width:]


def solution(mesh):
    in_specs = (
        P(("groups", "outer"), "inner", "head", None),
        P(("groups", "outer"), "inner", None),
        P(("groups", "outer"), "inner", None),
        P(("groups", "outer"), "inner", "head", None),
        P(("groups", "outer"), "head", "inner"),
        P(("groups", "outer"), "inner", "head", None),
        P(("groups", "outer"), None),
    )
    out_specs = (
        P(("groups", "outer"), "inner", "head", None),
        P(("groups", "outer"), "inner", None),
        P(("groups", "outer"), "inner", None),
    )
    return jax.shard_map(body, mesh=mesh, in_specs=in_specs, out_specs=out_specs, check_vma=False)
```

```python
import functools
import math

import jax
import jax.numpy as jnp
from jax import lax
from jax.experimental import pallas as pl
from jax.experimental.pallas import tpu as pltpu
from jax.sharding import PartitionSpec as P


LOG2E = math.log2(math.e)
NEAR = 2
BUNDLE = 2
CALLS = (2, 4, 2)
STAT_ROWS = 16


def split_stats(stats):
    high = lax.reduce_precision(stats, 8, 7)
    middle = lax.reduce_precision(stats - high, 8, 7)
    low = stats - high - middle
    pad = ((0, STAT_ROWS - stats.shape[0]), (0, 0))
    return [jnp.pad(a, pad).astype(jnp.bfloat16) for a in (high, middle, low)]


def kernel(first, count, heads, toks, order, where, mine, theirs, *refs):
    fresh = first == 0
    dq, dkv = refs if fresh else refs[1:]
    rows = heads * toks
    payload = 2 * rows + 3 * STAT_ROWS
    span_rows = toks // 2
    width = mine.shape[1]
    keys = NEAR * payload
    ring = (mine.shape[0] - keys) // toks
    scale = 1.0 / math.sqrt(width)
    place, core = where[0], where[1]
    step, member = place // NEAR, place % NEAR
    token = lax.broadcasted_iota(jnp.int32, (toks, toks), 1)
    row = lax.broadcasted_iota(jnp.int32, (toks, toks), 0)
    key_row, token_row = row % span_rows, token % span_rows
    nt = (((1,), (1,)), ((), ()))
    tn = (((0,), (0,)), ((), ()))
    if fresh:
        dq[...] = jnp.zeros_like(dq)
    else:
        dq[...] = refs[0][...]

    def one_block(index, carry):
        turn = first + index
        ahead = jnp.where(core == 0, turn - (ring // 2 - 1), ring // 2 - turn)
        block = lax.rem(step + ahead + ring, ring)
        chip = block * NEAR + member
        start = pl.multiple_of(keys + block * toks, STAT_ROWS)
        a, b = mine[pl.ds(start, toks)], theirs[pl.ds(start, toks)]
        low, high = jnp.where(core == 0, a, b), jnp.where(core == 0, b, a)
        k = jnp.concatenate([low[:span_rows], high[:span_rows]])
        v = jnp.concatenate([low[span_rows:], high[span_rows:]])
        key_span = jnp.where(row < span_rows, order[2 * chip], order[2 * chip + 1])
        key_pos = key_span * span_rows + key_row
        dk = jnp.zeros((toks, width), jnp.float32)
        dv = jnp.zeros((toks, width), jnp.float32)
        for near in range(NEAR):
            near_chip = step * NEAR + (member ^ near)
            span = jnp.where(token < span_rows, order[2 * near_chip], order[2 * near_chip + 1])
            visible = key_pos <= span * span_rows + token_row
            base = near * payload
            for part, source in ((near, mine), (NEAR + near, theirs)):
                q = source[base : base + rows]
                d = source[base + rows : base + 2 * rows]
                stat = [
                    source[base + 2 * rows + i * STAT_ROWS : base + 2 * rows + (i + 1) * STAT_ROWS]
                    for i in range(3)
                ]
                stat = sum(x.astype(jnp.float32) for x in stat)
                s = lax.dot_general(k, q, nt, preferred_element_type=jnp.float32)
                g = lax.dot_general(v, d, nt, preferred_element_type=jnp.float32)
                probs, grads = [], []
                for h in range(heads):
                    cols = slice(h * toks, (h + 1) * toks)
                    p = jnp.exp2(s[:, cols] * (scale * LOG2E) - stat[h : h + 1])
                    p = jnp.where(visible, p, 0.0)
                    probs.append(p.astype(jnp.bfloat16))
                    ds = p * (g[:, cols] - stat[heads + h : heads + h + 1]) * scale
                    grads.append(ds.astype(jnp.bfloat16))
                p = jnp.concatenate(probs, axis=1)
                ds = jnp.concatenate(grads, axis=1)
                dv = dv + jnp.dot(p, d, preferred_element_type=jnp.float32)
                dk = dk + jnp.dot(ds, q, preferred_element_type=jnp.float32)
                dq[part] += lax.dot_general(ds, k, tn, preferred_element_type=jnp.float32)
        dkv[index, :, :width] = dk
        dkv[index, :, width:] = dv
        return carry

    lax.fori_loop(0, count, one_block, 0)


def attention_grads(first, count, heads, toks, order, where, mine, theirs, dq):
    width = mine.shape[1]
    rows = heads * toks
    smem = pl.BlockSpec(memory_space=pltpu.SMEM)
    vmem = pl.BlockSpec(memory_space=pltpu.VMEM)
    operands = [order, where, mine, theirs] + ([] if dq is None else [dq])
    return pl.pallas_call(
        functools.partial(kernel, first, count, heads, toks),
        out_shape=(
            jax.ShapeDtypeStruct((2 * NEAR, rows, width), jnp.float32),
            jax.ShapeDtypeStruct((count, toks, 2 * width), jnp.float32),
        ),
        in_specs=[smem, smem] + [vmem] * (len(operands) - 2),
        out_specs=(vmem, vmem),
        input_output_aliases={} if dq is None else {len(operands) - 1: 0},
        compiler_params=pltpu.CompilerParams(vmem_limit_bytes=16 * 1024 * 1024),
        cost_estimate=pl.CostEstimate(
            flops=2 * 5 * 2 * NEAR * rows * count * toks * width,
            bytes_accessed=8 * rows * width * 4,
            transcendentals=2 * NEAR * rows * count * toks,
        ),
    )(*operands)


def body(queries, keys, values, out, log_total, d_out, span_order):
    size = lax.axis_size("inner")
    place = lax.axis_index("inner")
    core = lax.axis_index("head")
    toks, heads, width = queries.shape[1:]
    half = toks // 2
    rows = heads * toks

    def move(array, target):
        pairs = []
        for z in range(size):
            for c in range(2):
                to = target(z, c)
                if to is not None:
                    pairs.append((2 * z + c, 2 * (to[0] % size) + to[1]))
        return lax.ppermute(array, ("inner", "head"), pairs)

    def swap(z, c):
        return z, 1 - c

    def near(distance):
        return lambda z, c: (z ^ distance, c)

    delta = jnp.transpose(
        jnp.sum(out[0].astype(jnp.float32) * d_out[0].astype(jnp.float32), axis=-1)
    )
    payload = jnp.concatenate(
        [
            jnp.transpose(queries[0], (1, 0, 2)).reshape(rows, width),
            jnp.transpose(d_out[0], (1, 0, 2)).reshape(rows, width),
            *split_stats(jnp.concatenate([log_total[0] * LOG2E, delta])),
        ]
    )
    payloads = [payload] + [move(payload, near(i)) for i in range(1, NEAR)]

    kv = jnp.concatenate(
        [lax.dynamic_slice_in_dim(a[0], core * half, half, 0) for a in (keys, values)]
    )
    groups = [list(range(first, size, NEAR)) for first in range(NEAR)]
    kv = lax.all_gather(kv, "inner", axis_index_groups=groups, tiled=True)
    mine = jnp.concatenate([*payloads, kv])
    theirs = move(mine, swap)

    order = span_order[0]
    where = jnp.stack([place, core]).astype(jnp.int32)
    dq, parts, first = None, [], 0
    for count in CALLS:
        dq, part = attention_grads(first, count, heads, toks, order, where, mine, theirs, dq)
        parts += [part[i : i + BUNDLE] for i in range(0, count, BUNDLE)]
        first += count

    def hop(blocks):
        return lambda z, c: (z - blocks * NEAR, 0) if c == 0 else (z + blocks * NEAR, 1)

    total = parts[0].astype(jnp.bfloat16)
    for part in parts[1:]:
        total = move(total, hop(BUNDLE))
        sums = total.astype(jnp.float32) + part
        total = sums.astype(jnp.bfloat16)
    total = move(total[0], hop(1)).astype(jnp.float32) + sums[1]
    total = total.astype(jnp.bfloat16)
    one = move(total, lambda z, c: (z, 1) if c == 0 else (z + NEAR, 0))
    two = move(total, lambda z, c: None if c == 0 else (z + NEAR, 1))
    two = jnp.where(core == 0, total, two)
    dkv = (one.astype(jnp.float32) + two.astype(jnp.float32)).astype(jnp.bfloat16)

    dq_theirs = move(dq[NEAR:].astype(jnp.bfloat16), swap)
    dq_mine = dq[:NEAR] + dq_theirs.astype(jnp.float32)
    dq_back = [dq_mine[i].astype(jnp.bfloat16) for i in range(1, NEAR)]
    backs = [move(dq_back[i - 1], near(i)) for i in range(1, NEAR)]
    query_grad = dq_mine[0] + sum(back.astype(jnp.float32) for back in backs)
    query_grad = query_grad.astype(jnp.bfloat16).reshape(heads, toks, width)
    query_grad = jnp.transpose(query_grad, (1, 0, 2))
    return query_grad[None], dkv[None, :, :width], dkv[None, :, width:]


def solution(mesh):
    in_specs = (
        P(("groups", "outer"), "inner", "head", None),
        P(("groups", "outer"), "inner", None),
        P(("groups", "outer"), "inner", None),
        P(("groups", "outer"), "inner", "head", None),
        P(("groups", "outer"), "head", "inner"),
        P(("groups", "outer"), "inner", "head", None),
        P(("groups", "outer"), None),
    )
    out_specs = (
        P(("groups", "outer"), "inner", "head", None),
        P(("groups", "outer"), "inner", None),
        P(("groups", "outer"), "inner", None),
    )
    return jax.shard_map(body, mesh=mesh, in_specs=in_specs, out_specs=out_specs, check_vma=False)
```

```python
import functools
import math

import jax
import jax.numpy as jnp
from jax import lax
from jax.experimental import pallas as pl
from jax.experimental.pallas import tpu as pltpu
from jax.sharding import PartitionSpec as P


LOG2E = math.log2(math.e)
NEAR = 2
BUNDLE = 2
CALLS = (2, 4, 2)
STAT_ROWS = 16


def split_stats(stats):
    high = lax.reduce_precision(stats, 8, 7)
    middle = lax.reduce_precision(stats - high, 8, 7)
    low = stats - high - middle
    pad = ((0, STAT_ROWS - stats.shape[0]), (0, 0))
    return [jnp.pad(a, pad).astype(jnp.bfloat16) for a in (high, middle, low)]


def kernel(first, count, heads, toks, order, where, mine, theirs, *refs):
    fresh = first == 0
    dq, dkv = refs if fresh else refs[1:]
    rows = heads * toks
    payload = 2 * rows + 3 * STAT_ROWS
    span_rows = toks // 2
    width = mine.shape[1]
    keys = NEAR * payload
    ring = (mine.shape[0] - keys) // toks
    scale = 1.0 / math.sqrt(width)
    place, core = where[0], where[1]
    step, member = place // NEAR, place % NEAR
    role = lax.rem(core + step // BUNDLE, 2)
    token = lax.broadcasted_iota(jnp.int32, (toks, toks), 1)
    row = lax.broadcasted_iota(jnp.int32, (toks, toks), 0)
    key_row, token_row = row % span_rows, token % span_rows
    nt = (((1,), (1,)), ((), ()))
    tn = (((0,), (0,)), ((), ()))
    if fresh:
        dq[...] = jnp.zeros_like(dq)
    else:
        dq[...] = refs[0][...]

    def one_bundle(index, carry):
        ks, vs, positions = [], [], []
        for j in range(BUNDLE):
            turn = first + index * BUNDLE + j
            ahead = jnp.where(role == 0, turn - (ring // 2 - 1), ring // 2 - turn)
            block = lax.rem(step + ahead + ring, ring)
            chip = block * NEAR + member
            start = pl.multiple_of(keys + block * toks, STAT_ROWS)
            a, b = mine[pl.ds(start, toks)], theirs[pl.ds(start, toks)]
            first_span = lax.rem(block + step + core, 2) == 0
            low, high = jnp.where(first_span, a, b), jnp.where(first_span, b, a)
            ks += [low[:span_rows], high[:span_rows]]
            vs += [low[span_rows:], high[span_rows:]]
            key_span = jnp.where(row < span_rows, order[2 * chip], order[2 * chip + 1])
            positions.append(key_span * span_rows + key_row)
        k, v, key_pos = jnp.concatenate(ks), jnp.concatenate(vs), jnp.concatenate(positions)
        dk = jnp.zeros((BUNDLE * toks, width), jnp.float32)
        dv = jnp.zeros((BUNDLE * toks, width), jnp.float32)
        for near in range(NEAR):
            near_chip = step * NEAR + (member ^ near)
            span = jnp.where(token < span_rows, order[2 * near_chip], order[2 * near_chip + 1])
            query_pos = span * span_rows + token_row
            visible = key_pos <= jnp.concatenate([query_pos] * BUNDLE)
            base = near * payload
            for part, source in ((near, mine), (NEAR + near, theirs)):
                q = source[base : base + rows]
                d = source[base + rows : base + 2 * rows]
                stat = [
                    source[base + 2 * rows + i * STAT_ROWS : base + 2 * rows + (i + 1) * STAT_ROWS]
                    for i in range(3)
                ]
                stat = sum(x.astype(jnp.float32) for x in stat)
                s = lax.dot_general(k, q, nt, preferred_element_type=jnp.float32)
                g = lax.dot_general(v, d, nt, preferred_element_type=jnp.float32)
                probs, grads = [], []
                for h in range(heads):
                    cols = slice(h * toks, (h + 1) * toks)
                    p = jnp.exp2(s[:, cols] * (scale * LOG2E) - stat[h : h + 1])
                    p = jnp.where(visible, p, 0.0)
                    probs.append(p.astype(jnp.bfloat16))
                    ds = p * (g[:, cols] - stat[heads + h : heads + h + 1]) * scale
                    grads.append(ds.astype(jnp.bfloat16))
                p = jnp.concatenate(probs, axis=1)
                ds = jnp.concatenate(grads, axis=1)
                dv = dv + jnp.dot(p, d, preferred_element_type=jnp.float32)
                dk = dk + jnp.dot(ds, q, preferred_element_type=jnp.float32)
                dq[part] += lax.dot_general(ds, k, tn, preferred_element_type=jnp.float32)
        for j in range(BUNDLE):
            dkv[index * BUNDLE + j, :, :width] = dk[j * toks : (j + 1) * toks]
            dkv[index * BUNDLE + j, :, width:] = dv[j * toks : (j + 1) * toks]
        return carry

    lax.fori_loop(0, count // BUNDLE, one_bundle, 0)


def attention_grads(first, count, heads, toks, order, where, mine, theirs, dq):
    width = mine.shape[1]
    rows = heads * toks
    smem = pl.BlockSpec(memory_space=pltpu.SMEM)
    vmem = pl.BlockSpec(memory_space=pltpu.VMEM)
    operands = [order, where, mine, theirs] + ([] if dq is None else [dq])
    return pl.pallas_call(
        functools.partial(kernel, first, count, heads, toks),
        out_shape=(
            jax.ShapeDtypeStruct((2 * NEAR, rows, width), jnp.float32),
            jax.ShapeDtypeStruct((count, toks, 2 * width), jnp.float32),
        ),
        in_specs=[smem, smem] + [vmem] * (len(operands) - 2),
        out_specs=(vmem, vmem),
        input_output_aliases={} if dq is None else {len(operands) - 1: 0},
        compiler_params=pltpu.CompilerParams(vmem_limit_bytes=16 * 1024 * 1024),
        cost_estimate=pl.CostEstimate(
            flops=2 * 5 * 2 * NEAR * rows * count * toks * width,
            bytes_accessed=8 * rows * width * 4,
            transcendentals=2 * NEAR * rows * count * toks,
        ),
    )(*operands)


def body(queries, keys, values, out, log_total, d_out, span_order):
    size = lax.axis_size("inner")
    place = lax.axis_index("inner")
    core = lax.axis_index("head")
    toks, heads, width = queries.shape[1:]
    half = toks // 2
    rows = heads * toks

    def move(array, target):
        pairs = []
        for z in range(size):
            for c in range(2):
                to = target(z, c)
                if to is not None:
                    pairs.append((2 * z + c, 2 * (to[0] % size) + to[1]))
        return lax.ppermute(array, ("inner", "head"), pairs)

    def swap(z, c):
        return z, 1 - c

    def near(distance):
        return lambda z, c: (z ^ distance, c)

    delta = jnp.transpose(
        jnp.sum(out[0].astype(jnp.float32) * d_out[0].astype(jnp.float32), axis=-1)
    )
    payload = jnp.concatenate(
        [
            jnp.transpose(queries[0], (1, 0, 2)).reshape(rows, width),
            jnp.transpose(d_out[0], (1, 0, 2)).reshape(rows, width),
            *split_stats(jnp.concatenate([log_total[0] * LOG2E, delta])),
        ]
    )
    payloads = [payload] + [move(payload, near(i)) for i in range(1, NEAR)]

    kv = jnp.concatenate(
        [lax.dynamic_slice_in_dim(a[0], core * half, half, 0) for a in (keys, values)]
    )
    groups = [
        [2 * z + (z // NEAR + first) % 2 for z in range(chip, size, NEAR)]
        for chip in range(NEAR)
        for first in range(2)
    ]
    kv = lax.all_gather(kv, ("inner", "head"), axis_index_groups=groups, tiled=True)
    mine = jnp.concatenate([*payloads, kv])
    theirs = move(mine, swap)

    order = span_order[0]
    where = jnp.stack([place, core]).astype(jnp.int32)
    dq, parts, first = None, [], 0
    for count in CALLS:
        dq, part = attention_grads(first, count, heads, toks, order, where, mine, theirs, dq)
        parts += [part[i : i + BUNDLE] for i in range(0, count, BUNDLE)]
        first += count

    def role_of(z, c):
        return (c + z // NEAR // BUNDLE) % 2

    def hop(blocks):
        def target(z, c):
            role = role_of(z, c)
            z = (z + (blocks if role else -blocks) * NEAR) % size
            return z, role_of(z, role)

        return target

    def last_one(z, c):
        after = (z + NEAR) % size
        return (after, role_of(after, 0)) if role_of(z, c) else (z, 1 - c)

    def last_two(z, c):
        return hop(1)(z, c) if role_of(z, c) else None

    total = parts[0].astype(jnp.bfloat16)
    for part in parts[1:]:
        total = move(total, hop(BUNDLE))
        sums = total.astype(jnp.float32) + part
        total = sums.astype(jnp.bfloat16)
    total = move(total[0], hop(1)).astype(jnp.float32) + sums[1]
    total = total.astype(jnp.bfloat16)
    one = move(total, last_one)
    two = move(total, last_two)
    two = jnp.where(role_of(place, core) == 0, total, two)
    dkv = (one.astype(jnp.float32) + two.astype(jnp.float32)).astype(jnp.bfloat16)

    dq_theirs = move(dq[NEAR:].astype(jnp.bfloat16), swap)
    dq_mine = dq[:NEAR] + dq_theirs.astype(jnp.float32)
    dq_back = [dq_mine[i].astype(jnp.bfloat16) for i in range(1, NEAR)]
    backs = [move(dq_back[i - 1], near(i)) for i in range(1, NEAR)]
    query_grad = dq_mine[0] + sum(back.astype(jnp.float32) for back in backs)
    query_grad = query_grad.astype(jnp.bfloat16).reshape(heads, toks, width)
    query_grad = jnp.transpose(query_grad, (1, 0, 2))
    return query_grad[None], dkv[None, :, :width], dkv[None, :, width:]


def solution(mesh):
    in_specs = (
        P(("groups", "outer"), "inner", "head", None),
        P(("groups", "outer"), "inner", None),
        P(("groups", "outer"), "inner", None),
        P(("groups", "outer"), "inner", "head", None),
        P(("groups", "outer"), "head", "inner"),
        P(("groups", "outer"), "inner", "head", None),
        P(("groups", "outer"), None),
    )
    out_specs = (
        P(("groups", "outer"), "inner", "head", None),
        P(("groups", "outer"), "inner", None),
        P(("groups", "outer"), "inner", None),
    )
    return jax.shard_map(body, mesh=mesh, in_specs=in_specs, out_specs=out_specs, check_vma=False)
```

```python
import functools
import math

import jax
import jax.numpy as jnp
from jax import lax
from jax.experimental import pallas as pl
from jax.experimental.pallas import tpu as pltpu
from jax.sharding import PartitionSpec as P


LOG2E = math.log2(math.e)
NEAR = 2
BUNDLE = 2
CALLS = (2, 4, 2)
STAT_ROWS = 16


def split_stats(stats):
    high = lax.reduce_precision(stats, 8, 7)
    middle = lax.reduce_precision(stats - high, 8, 7)
    low = stats - high - middle
    pad = ((0, STAT_ROWS - stats.shape[0]), (0, 0))
    return [jnp.pad(a, pad).astype(jnp.bfloat16) for a in (high, middle, low)]


def kernel(first, count, heads, toks, order, where, mine, theirs, *refs):
    fresh = first == 0
    dq, dkv = refs if fresh else refs[1:]
    rows = heads * toks
    payload = 2 * rows + 3 * STAT_ROWS
    span_rows = toks // 2
    width = mine.shape[1]
    keys = NEAR * payload
    ring = (mine.shape[0] - keys) // toks
    scale = 1.0 / math.sqrt(width)
    place, core = where[0], where[1]
    step, member = place // NEAR, place % NEAR
    role = lax.rem(core + step // BUNDLE, 2)
    token = lax.broadcasted_iota(jnp.int32, (toks, toks), 1)
    row = lax.broadcasted_iota(jnp.int32, (toks, toks), 0)
    key_row, token_row = row % span_rows, token % span_rows
    nt = (((1,), (1,)), ((), ()))
    tn = (((0,), (0,)), ((), ()))
    if fresh:
        dq[...] = jnp.zeros_like(dq)
    else:
        dq[...] = refs[0][...]

    def one_bundle(index, carry):
        ks, vs, positions = [], [], []
        for j in range(BUNDLE):
            turn = first + index * BUNDLE + j
            ahead = jnp.where(role == 0, turn - (ring // 2 - 1), ring // 2 - turn)
            block = lax.rem(step + ahead + ring, ring)
            chip = block * NEAR + member
            start = pl.multiple_of(keys + block * toks, STAT_ROWS)
            a, b = mine[pl.ds(start, toks)], theirs[pl.ds(start, toks)]
            first_span = lax.rem(block + step + core, 2) == 0
            low, high = jnp.where(first_span, a, b), jnp.where(first_span, b, a)
            ks += [low[:span_rows], high[:span_rows]]
            vs += [low[span_rows:], high[span_rows:]]
            key_span = jnp.where(row < span_rows, order[2 * chip], order[2 * chip + 1])
            positions.append(key_span * span_rows + key_row)
        k, v, key_pos = jnp.concatenate(ks), jnp.concatenate(vs), jnp.concatenate(positions)
        dk = jnp.zeros((BUNDLE * toks, width), jnp.float32)
        dv = jnp.zeros((BUNDLE * toks, width), jnp.float32)
        for near in range(NEAR):
            near_chip = step * NEAR + (member ^ near)
            span = jnp.where(token < span_rows, order[2 * near_chip], order[2 * near_chip + 1])
            query_pos = span * span_rows + token_row
            visible = key_pos <= jnp.concatenate([query_pos] * BUNDLE)
            base = near * payload
            for part, source in ((near, mine), (NEAR + near, theirs)):
                q = source[base : base + rows]
                d = source[base + rows : base + 2 * rows]
                stat = [
                    source[base + 2 * rows + i * STAT_ROWS : base + 2 * rows + (i + 1) * STAT_ROWS]
                    for i in range(3)
                ]
                stat = sum(x.astype(jnp.float32) for x in stat)
                s = lax.dot_general(k, q, nt, preferred_element_type=jnp.float32)
                g = lax.dot_general(v, d, nt, preferred_element_type=jnp.float32)
                probs, grads = [], []
                for h in range(heads):
                    cols = slice(h * toks, (h + 1) * toks)
                    p = jnp.exp2(s[:, cols] * (scale * LOG2E) - stat[h : h + 1])
                    p = jnp.where(visible, p, 0.0)
                    probs.append(p.astype(jnp.bfloat16))
                    ds = p * (g[:, cols] - stat[heads + h : heads + h + 1]) * scale
                    grads.append(ds.astype(jnp.bfloat16))
                p = jnp.concatenate(probs, axis=1)
                ds = jnp.concatenate(grads, axis=1)
                dv = dv + jnp.dot(p, d, preferred_element_type=jnp.float32)
                dk = dk + jnp.dot(ds, q, preferred_element_type=jnp.float32)
                dq[part] += lax.dot_general(ds, k, tn, preferred_element_type=jnp.float32)
        for j in range(BUNDLE):
            dkv[index * BUNDLE + j, :, :width] = dk[j * toks : (j + 1) * toks]
            dkv[index * BUNDLE + j, :, width:] = dv[j * toks : (j + 1) * toks]
        return carry

    lax.fori_loop(0, count // BUNDLE, one_bundle, 0)


def attention_grads(first, count, heads, toks, order, where, mine, theirs, dq):
    width = mine.shape[1]
    rows = heads * toks
    smem = pl.BlockSpec(memory_space=pltpu.SMEM)
    vmem = pl.BlockSpec(memory_space=pltpu.VMEM)
    operands = [order, where, mine, theirs] + ([] if dq is None else [dq])
    return pl.pallas_call(
        functools.partial(kernel, first, count, heads, toks),
        out_shape=(
            jax.ShapeDtypeStruct((2 * NEAR, rows, width), jnp.float32),
            jax.ShapeDtypeStruct((count, toks, 2 * width), jnp.float32),
        ),
        in_specs=[smem, smem] + [vmem] * (len(operands) - 2),
        out_specs=(vmem, vmem),
        input_output_aliases={} if dq is None else {len(operands) - 1: 0},
        compiler_params=pltpu.CompilerParams(vmem_limit_bytes=16 * 1024 * 1024),
        cost_estimate=pl.CostEstimate(
            flops=2 * 5 * 2 * NEAR * rows * count * toks * width,
            bytes_accessed=8 * rows * width * 4,
            transcendentals=2 * NEAR * rows * count * toks,
        ),
    )(*operands)


def body(queries, keys, values, out, log_total, d_out, span_order):
    size = lax.axis_size("inner")
    place = lax.axis_index("inner")
    core = lax.axis_index("head")
    toks, heads, width = queries.shape[1:]
    half = toks // 2
    rows = heads * toks

    def move(array, target):
        pairs = []
        for z in range(size):
            for c in range(2):
                to = target(z, c)
                if to is not None:
                    pairs.append((2 * z + c, 2 * (to[0] % size) + to[1]))
        return lax.ppermute(array, ("inner", "head"), pairs)

    def swap(z, c):
        return z, 1 - c

    def near(distance):
        return lambda z, c: (z ^ distance, c)

    delta = jnp.transpose(
        jnp.sum(out[0].astype(jnp.float32) * d_out[0].astype(jnp.float32), axis=-1)
    )
    payload = jnp.concatenate(
        [
            jnp.transpose(queries[0], (1, 0, 2)).reshape(rows, width),
            jnp.transpose(d_out[0], (1, 0, 2)).reshape(rows, width),
            *split_stats(jnp.concatenate([log_total[0] * LOG2E, delta])),
        ]
    )
    payloads = [payload] + [move(payload, near(i)) for i in range(1, NEAR)]

    kv = jnp.concatenate(
        [lax.dynamic_slice_in_dim(a[0], core * half, half, 0) for a in (keys, values)]
    )
    groups = [
        [2 * z + (z // NEAR + first) % 2 for z in range(chip, size, NEAR)]
        for chip in range(NEAR)
        for first in range(2)
    ]
    kv = lax.all_gather(kv, ("inner", "head"), axis_index_groups=groups, tiled=True)
    mine = jnp.concatenate([*payloads, kv])
    theirs = move(mine, swap)

    order = span_order[0]
    where = jnp.stack([place, core]).astype(jnp.int32)
    dq, parts, first = None, [], 0
    for count in CALLS:
        dq, part = attention_grads(first, count, heads, toks, order, where, mine, theirs, dq)
        parts += [part[i : i + BUNDLE] for i in range(0, count, BUNDLE)]
        first += count

    def role_of(z, c):
        return (c + z // NEAR // BUNDLE) % 2

    def hop(blocks):
        def target(z, c):
            role = role_of(z, c)
            z = (z + (blocks if role else -blocks) * NEAR) % size
            return z, role_of(z, role)

        return target

    total = parts[0].astype(jnp.bfloat16)
    for part in parts[1:]:
        total = move(total, hop(BUNDLE))
        total = (total.astype(jnp.float32) + part).astype(jnp.bfloat16)

    def home(role0, role1):
        def target(z, c):
            to = role1 if role_of(z, c) else role0
            if to is None:
                return None
            z = (z + to[0] * NEAR) % size
            return z, role_of(z, to[1])

        return target

    down = role_of(place, core) == 0
    away, beside = total[0], total[1]
    first = move(away, home((-1, 1), (2, 0)))
    second = move(away, home((-1, 0), (2, 1)))
    third = move(beside, home((0, 1), (1, 0)))
    fourth = move(beside, home(None, (1, 1)))
    pieces = (
        jnp.where(down, beside, third),
        jnp.where(down, second, first),
        jnp.where(down, third, fourth),
        jnp.where(down, first, second),
    )
    dkv = sum(piece.astype(jnp.float32) for piece in pieces).astype(jnp.bfloat16)

    dq_theirs = move(dq[NEAR:].astype(jnp.bfloat16), swap)
    dq_mine = dq[:NEAR] + dq_theirs.astype(jnp.float32)
    dq_back = [dq_mine[i].astype(jnp.bfloat16) for i in range(1, NEAR)]
    backs = [move(dq_back[i - 1], near(i)) for i in range(1, NEAR)]
    query_grad = dq_mine[0] + sum(back.astype(jnp.float32) for back in backs)
    query_grad = query_grad.astype(jnp.bfloat16).reshape(heads, toks, width)
    query_grad = jnp.transpose(query_grad, (1, 0, 2))
    return query_grad[None], dkv[None, :, :width], dkv[None, :, width:]


def solution(mesh):
    in_specs = (
        P(("groups", "outer"), "inner", "head", None),
        P(("groups", "outer"), "inner", None),
        P(("groups", "outer"), "inner", None),
        P(("groups", "outer"), "inner", "head", None),
        P(("groups", "outer"), "head", "inner"),
        P(("groups", "outer"), "inner", "head", None),
        P(("groups", "outer"), None),
    )
    out_specs = (
        P(("groups", "outer"), "inner", "head", None),
        P(("groups", "outer"), "inner", None),
        P(("groups", "outer"), "inner", None),
    )
    return jax.shard_map(body, mesh=mesh, in_specs=in_specs, out_specs=out_specs, check_vma=False)
```

```python
import functools
import math

import jax
import jax.numpy as jnp
from jax import lax
from jax.experimental import pallas as pl
from jax.experimental.pallas import tpu as pltpu
from jax.sharding import PartitionSpec as P


LOG2E = math.log2(math.e)
NEAR = 2
BUNDLE = 2
CALLS = (2, 4, 2)
STAT_ROWS = 16


def split_stats(stats):
    high = lax.reduce_precision(stats, 8, 7)
    middle = lax.reduce_precision(stats - high, 8, 7)
    low = stats - high - middle
    pad = ((0, STAT_ROWS - stats.shape[0]), (0, 0))
    return [jnp.pad(a, pad).astype(jnp.bfloat16) for a in (high, middle, low)]


def kernel(first, count, heads, toks, order, where, mine, theirs, *refs):
    fresh = first == 0
    dq, *parts = refs if fresh else refs[1:]
    rows = heads * toks
    payload = 2 * rows + 3 * STAT_ROWS
    span_rows = toks // 2
    width = mine.shape[1]
    keys = NEAR * payload
    ring = (mine.shape[0] - keys) // toks
    scale = 1.0 / math.sqrt(width)
    place, core = where[0], where[1]
    step, member = place // NEAR, place % NEAR
    role = lax.rem(core + step // BUNDLE, 2)
    token = lax.broadcasted_iota(jnp.int32, (toks, toks), 1)
    row = lax.broadcasted_iota(jnp.int32, (toks, toks), 0)
    key_row, token_row = row % span_rows, token % span_rows
    nt = (((1,), (1,)), ((), ()))
    tn = (((0,), (0,)), ((), ()))
    if fresh:
        dq[...] = jnp.zeros_like(dq)
    else:
        dq[...] = refs[0][...]

    def one_bundle(index):
        ks, vs, positions = [], [], []
        for j in range(BUNDLE):
            turn = first + index * BUNDLE + j
            ahead = jnp.where(role == 0, turn - (ring // 2 - 1), ring // 2 - turn)
            block = lax.rem(step + ahead + ring, ring)
            chip = block * NEAR + member
            start = pl.multiple_of(keys + block * toks, STAT_ROWS)
            a, b = mine[pl.ds(start, toks)], theirs[pl.ds(start, toks)]
            first_span = lax.rem(block + step + core, 2) == 0
            low, high = jnp.where(first_span, a, b), jnp.where(first_span, b, a)
            ks += [low[:span_rows], high[:span_rows]]
            vs += [low[span_rows:], high[span_rows:]]
            key_span = jnp.where(row < span_rows, order[2 * chip], order[2 * chip + 1])
            positions.append(key_span * span_rows + key_row)
        k, v, key_pos = jnp.concatenate(ks), jnp.concatenate(vs), jnp.concatenate(positions)
        dk = jnp.zeros((BUNDLE * toks, width), jnp.float32)
        dv = jnp.zeros((BUNDLE * toks, width), jnp.float32)
        for near in range(NEAR):
            near_chip = step * NEAR + (member ^ near)
            span = jnp.where(token < span_rows, order[2 * near_chip], order[2 * near_chip + 1])
            query_pos = span * span_rows + token_row
            visible = key_pos <= jnp.concatenate([query_pos] * BUNDLE)
            base = near * payload
            for part, source in ((near, mine), (NEAR + near, theirs)):
                q = source[base : base + rows]
                d = source[base + rows : base + 2 * rows]
                stat = [
                    source[base + 2 * rows + i * STAT_ROWS : base + 2 * rows + (i + 1) * STAT_ROWS]
                    for i in range(3)
                ]
                stat = sum(x.astype(jnp.float32) for x in stat)
                s = lax.dot_general(k, q, nt, preferred_element_type=jnp.float32)
                g = lax.dot_general(v, d, nt, preferred_element_type=jnp.float32)
                probs, grads = [], []
                for h in range(heads):
                    cols = slice(h * toks, (h + 1) * toks)
                    p = jnp.exp2(s[:, cols] * (scale * LOG2E) - stat[h : h + 1])
                    p = jnp.where(visible, p, 0.0)
                    probs.append(p.astype(jnp.bfloat16))
                    ds = p * (g[:, cols] - stat[heads + h : heads + h + 1]) * scale
                    grads.append(ds.astype(jnp.bfloat16))
                p = jnp.concatenate(probs, axis=1)
                ds = jnp.concatenate(grads, axis=1)
                dv = dv + jnp.dot(p, d, preferred_element_type=jnp.float32)
                dk = dk + jnp.dot(ds, q, preferred_element_type=jnp.float32)
                dq[part] += lax.dot_general(ds, k, tn, preferred_element_type=jnp.float32)
        for j in range(BUNDLE):
            parts[index * BUNDLE + j][:, :width] = dk[j * toks : (j + 1) * toks]
            parts[index * BUNDLE + j][:, width:] = dv[j * toks : (j + 1) * toks]

    for index in range(count // BUNDLE):
        one_bundle(index)


def attention_grads(first, count, heads, toks, order, where, mine, theirs, dq):
    width = mine.shape[1]
    rows = heads * toks
    smem = pl.BlockSpec(memory_space=pltpu.SMEM)
    vmem = pl.BlockSpec(memory_space=pltpu.VMEM)
    operands = [order, where, mine, theirs] + ([] if dq is None else [dq])
    return pl.pallas_call(
        functools.partial(kernel, first, count, heads, toks),
        out_shape=(
            jax.ShapeDtypeStruct((2 * NEAR, rows, width), jnp.float32),
            *[jax.ShapeDtypeStruct((toks, 2 * width), jnp.float32)] * count,
        ),
        in_specs=[smem, smem] + [vmem] * (len(operands) - 2),
        out_specs=(vmem,) * (1 + count),
        input_output_aliases={} if dq is None else {len(operands) - 1: 0},
        compiler_params=pltpu.CompilerParams(vmem_limit_bytes=16 * 1024 * 1024),
        cost_estimate=pl.CostEstimate(
            flops=2 * 5 * 2 * NEAR * rows * count * toks * width,
            bytes_accessed=8 * rows * width * 4,
            transcendentals=2 * NEAR * rows * count * toks,
        ),
    )(*operands)


def body(queries, keys, values, out, log_total, d_out, span_order):
    size = lax.axis_size("inner")
    place = lax.axis_index("inner")
    core = lax.axis_index("head")
    toks, heads, width = queries.shape[1:]
    half = toks // 2
    rows = heads * toks

    def move(array, target):
        pairs = []
        for z in range(size):
            for c in range(2):
                to = target(z, c)
                if to is not None:
                    pairs.append((2 * z + c, 2 * (to[0] % size) + to[1]))
        return lax.ppermute(array, ("inner", "head"), pairs)

    def swap(z, c):
        return z, 1 - c

    def near(distance):
        return lambda z, c: (z ^ distance, c)

    delta = jnp.transpose(
        jnp.sum(out[0].astype(jnp.float32) * d_out[0].astype(jnp.float32), axis=-1)
    )
    payload = jnp.concatenate(
        [
            jnp.transpose(queries[0], (1, 0, 2)).reshape(rows, width),
            jnp.transpose(d_out[0], (1, 0, 2)).reshape(rows, width),
            *split_stats(jnp.concatenate([log_total[0] * LOG2E, delta])),
        ]
    )
    payloads = [payload] + [move(payload, near(i)) for i in range(1, NEAR)]

    kv = jnp.concatenate(
        [lax.dynamic_slice_in_dim(a[0], core * half, half, 0) for a in (keys, values)]
    )
    groups = [
        [2 * z + (z // NEAR + first) % 2 for z in range(chip, size, NEAR)]
        for chip in range(NEAR)
        for first in range(2)
    ]
    kv = lax.all_gather(kv, ("inner", "head"), axis_index_groups=groups, tiled=True)
    mine = jnp.concatenate([*payloads, kv])
    theirs = move(mine, swap)

    order = span_order[0]
    where = jnp.stack([place, core]).astype(jnp.int32)
    dq, parts, first = None, [], 0
    for count in CALLS:
        dq, *part = attention_grads(first, count, heads, toks, order, where, mine, theirs, dq)
        parts += part
        first += count

    def role_of(z, c):
        return (c + z // NEAR // BUNDLE) % 2

    def hop(blocks):
        def target(z, c):
            role = role_of(z, c)
            z = (z + (blocks if role else -blocks) * NEAR) % size
            return z, role_of(z, role)

        return target

    def last_one(z, c):
        after = (z + NEAR) % size
        return (after, role_of(after, 0)) if role_of(z, c) else (z, 1 - c)

    def last_two(z, c):
        return hop(1)(z, c) if role_of(z, c) else None

    totals = [parts[j].astype(jnp.bfloat16) for j in range(BUNDLE)]
    for turn in range(len(parts) // BUNDLE - 1):
        moved = [move(totals[j], hop(BUNDLE)) for j in range(BUNDLE)]
        for j in range(BUNDLE):
            sums = moved[j].astype(jnp.float32) + parts[(turn + 1) * BUNDLE + j]
            totals[j] = sums.astype(jnp.bfloat16)
    sums = lax.optimization_barrier(sums)
    total = move(totals[0], hop(1)).astype(jnp.float32) + sums
    total = total.astype(jnp.bfloat16)
    one = move(total, last_one)
    two = move(total, last_two)
    two = jnp.where(role_of(place, core) == 0, total, two)
    dkv = (one.astype(jnp.float32) + two.astype(jnp.float32)).astype(jnp.bfloat16)

    dq_theirs = move(dq[NEAR:].astype(jnp.bfloat16), swap)
    dq_mine = dq[:NEAR] + dq_theirs.astype(jnp.float32)
    dq_back = [dq_mine[i].astype(jnp.bfloat16) for i in range(1, NEAR)]
    backs = [move(dq_back[i - 1], near(i)) for i in range(1, NEAR)]
    query_grad = dq_mine[0] + sum(back.astype(jnp.float32) for back in backs)
    query_grad = query_grad.astype(jnp.bfloat16).reshape(heads, toks, width)
    query_grad = jnp.transpose(query_grad, (1, 0, 2))
    return query_grad[None], dkv[None, :, :width], dkv[None, :, width:]


def solution(mesh):
    in_specs = (
        P(("groups", "outer"), "inner", "head", None),
        P(("groups", "outer"), "inner", None),
        P(("groups", "outer"), "inner", None),
        P(("groups", "outer"), "inner", "head", None),
        P(("groups", "outer"), "head", "inner"),
        P(("groups", "outer"), "inner", "head", None),
        P(("groups", "outer"), None),
    )
    out_specs = (
        P(("groups", "outer"), "inner", "head", None),
        P(("groups", "outer"), "inner", None),
        P(("groups", "outer"), "inner", None),
    )
    return jax.shard_map(body, mesh=mesh, in_specs=in_specs, out_specs=out_specs, check_vma=False)
```

```python
import functools
import math

import jax
import jax.numpy as jnp
from jax import lax
from jax.experimental import pallas as pl
from jax.experimental.pallas import tpu as pltpu
from jax.sharding import PartitionSpec as P


LOG2E = math.log2(math.e)
NEAR = 2
BUNDLE = 2
CALLS = (2, 4, 2)
STAT_ROWS = 16


def rows_kernel(*refs):
    sources, payload, held, sems = refs[:4], refs[4], refs[5:9], refs[9]
    copies = [
        pltpu.make_async_copy(source, target, sems.at[i])
        for i, (source, target) in enumerate(zip(sources, held))
    ]
    for copy in copies:
        copy.start()
    for copy in copies:
        copy.wait()
    queries, d_out, out, log_total = held
    toks, heads, width = queries.shape
    rows = heads * toks
    deltas = []
    for h in range(heads):
        grad = d_out[:, h, :]
        payload[h * toks : (h + 1) * toks] = queries[:, h, :]
        payload[rows + h * toks : rows + (h + 1) * toks] = grad
        product = out[:, h, :].astype(jnp.float32) * grad.astype(jnp.float32)
        deltas.append(jnp.sum(product.T, axis=0, keepdims=True))
    rest = jnp.concatenate([log_total[...] * LOG2E, *deltas])
    rest = jnp.concatenate([rest, jnp.zeros((STAT_ROWS - 2 * heads, width), jnp.float32)])
    for i in range(3):
        term = rest.astype(jnp.bfloat16)
        payload[2 * rows + i * STAT_ROWS : 2 * rows + (i + 1) * STAT_ROWS] = term
        rest = rest - term.astype(jnp.float32)


def own_rows(*arrays):
    toks, heads, width = arrays[0].shape
    return pl.pallas_call(
        rows_kernel,
        out_shape=jax.ShapeDtypeStruct((2 * heads * toks + 3 * STAT_ROWS, width), jnp.bfloat16),
        in_specs=[pl.BlockSpec(memory_space=pltpu.HBM)] * len(arrays),
        out_specs=pl.BlockSpec(memory_space=pltpu.VMEM),
        scratch_shapes=[pltpu.VMEM(a.shape, a.dtype) for a in arrays]
        + [pltpu.SemaphoreType.DMA((len(arrays),))],
        compiler_params=pltpu.CompilerParams(vmem_limit_bytes=63 * 1024 * 1024),
        cost_estimate=pl.CostEstimate(
            flops=4 * heads * toks * width,
            bytes_accessed=10 * heads * toks * width,
            transcendentals=0,
        ),
    )(*arrays)


def kernel(first, count, heads, toks, order, where, mine, theirs, *refs):
    fresh = first == 0
    dq, dkv = refs if fresh else refs[1:]
    rows = heads * toks
    payload = 2 * rows + 3 * STAT_ROWS
    span_rows = toks // 2
    width = mine.shape[1]
    keys = NEAR * payload
    ring = (mine.shape[0] - keys) // toks
    scale = 1.0 / math.sqrt(width)
    place, core = where[0], where[1]
    step, member = place // NEAR, place % NEAR
    role = lax.rem(core + step // BUNDLE, 2)
    token = lax.broadcasted_iota(jnp.int32, (toks, toks), 1)
    row = lax.broadcasted_iota(jnp.int32, (toks, toks), 0)
    key_row, token_row = row % span_rows, token % span_rows
    nt = (((1,), (1,)), ((), ()))
    tn = (((0,), (0,)), ((), ()))

    def one_bundle(index):
        ks, vs, positions = [], [], []
        for j in range(BUNDLE):
            turn = first + index * BUNDLE + j
            ahead = jnp.where(role == 0, turn - (ring // 2 - 1), ring // 2 - turn)
            block = lax.rem(step + ahead + ring, ring)
            chip = block * NEAR + member
            start = pl.multiple_of(keys + block * toks, STAT_ROWS)
            a, b = mine[pl.ds(start, toks)], theirs[pl.ds(start, toks)]
            first_span = lax.rem(block + step + core, 2) == 0
            low, high = jnp.where(first_span, a, b), jnp.where(first_span, b, a)
            ks += [low[:span_rows], high[:span_rows]]
            vs += [low[span_rows:], high[span_rows:]]
            key_span = jnp.where(row < span_rows, order[2 * chip], order[2 * chip + 1])
            positions.append(key_span * span_rows + key_row)
        k, v, key_pos = jnp.concatenate(ks), jnp.concatenate(vs), jnp.concatenate(positions)
        dk = jnp.zeros((BUNDLE * toks, width), jnp.float32)
        dv = jnp.zeros((BUNDLE * toks, width), jnp.float32)
        for near in range(NEAR):
            near_chip = step * NEAR + (member ^ near)
            span = jnp.where(token < span_rows, order[2 * near_chip], order[2 * near_chip + 1])
            query_pos = span * span_rows + token_row
            visible = key_pos <= jnp.concatenate([query_pos] * BUNDLE)
            base = near * payload
            for part, source in ((near, mine), (NEAR + near, theirs)):
                q = source[base : base + rows]
                d = source[base + rows : base + 2 * rows]
                stat = [
                    source[base + 2 * rows + i * STAT_ROWS : base + 2 * rows + (i + 1) * STAT_ROWS]
                    for i in range(3)
                ]
                stat = sum(x.astype(jnp.float32) for x in stat)
                s = lax.dot_general(k, q, nt, preferred_element_type=jnp.float32)
                g = lax.dot_general(v, d, nt, preferred_element_type=jnp.float32)
                probs, grads = [], []
                for h in range(heads):
                    cols = slice(h * toks, (h + 1) * toks)
                    p = jnp.exp2(s[:, cols] * (scale * LOG2E) - stat[h : h + 1])
                    p = jnp.where(visible, p, 0.0)
                    probs.append(p.astype(jnp.bfloat16))
                    ds = p * (g[:, cols] - stat[heads + h : heads + h + 1]) * scale
                    grads.append(ds.astype(jnp.bfloat16))
                p = jnp.concatenate(probs, axis=1)
                ds = jnp.concatenate(grads, axis=1)
                dv = dv + jnp.dot(p, d, preferred_element_type=jnp.float32)
                dk = dk + jnp.dot(ds, q, preferred_element_type=jnp.float32)
                dq_part = lax.dot_general(ds, k, tn, preferred_element_type=jnp.float32)
                if index > 0:
                    dq_part += dq[part]
                elif not fresh:
                    dq_part += refs[0][part]
                dq[part] = dq_part
        for j in range(BUNDLE):
            dkv[index * BUNDLE + j, :, :width] = dk[j * toks : (j + 1) * toks]
            dkv[index * BUNDLE + j, :, width:] = dv[j * toks : (j + 1) * toks]

    for index in range(count // BUNDLE):
        one_bundle(index)


def attention_grads(first, count, heads, toks, order, where, mine, theirs, dq):
    width = mine.shape[1]
    rows = heads * toks
    smem = pl.BlockSpec(memory_space=pltpu.SMEM)
    vmem = pl.BlockSpec(memory_space=pltpu.VMEM)
    operands = [order, where, mine, theirs] + ([] if dq is None else [dq])
    return pl.pallas_call(
        functools.partial(kernel, first, count, heads, toks),
        out_shape=(
            jax.ShapeDtypeStruct((2 * NEAR, rows, width), jnp.float32),
            jax.ShapeDtypeStruct((count, toks, 2 * width), jnp.float32),
        ),
        in_specs=[smem, smem] + [vmem] * (len(operands) - 2),
        out_specs=(vmem, vmem),
        input_output_aliases={} if dq is None else {len(operands) - 1: 0},
        compiler_params=pltpu.CompilerParams(vmem_limit_bytes=16 * 1024 * 1024),
        cost_estimate=pl.CostEstimate(
            flops=2 * 5 * 2 * NEAR * rows * count * toks * width,
            bytes_accessed=8 * rows * width * 4,
            transcendentals=2 * NEAR * rows * count * toks,
        ),
    )(*operands)


def body(queries, keys, values, out, log_total, d_out, span_order):
    size = lax.axis_size("inner")
    place = lax.axis_index("inner")
    core = lax.axis_index("head")
    toks, heads, width = queries.shape[1:]
    half = toks // 2

    def move(array, target):
        pairs = []
        for z in range(size):
            for c in range(2):
                to = target(z, c)
                if to is not None:
                    pairs.append((2 * z + c, 2 * (to[0] % size) + to[1]))
        return lax.ppermute(array, ("inner", "head"), pairs)

    def swap(z, c):
        return z, 1 - c

    def near(distance):
        return lambda z, c: (z ^ distance, c)

    payload = own_rows(queries[0], d_out[0], out[0], log_total[0])
    payloads = [payload] + [move(payload, near(i)) for i in range(1, NEAR)]

    kv = jnp.concatenate(
        [lax.dynamic_slice_in_dim(a[0], core * half, half, 0) for a in (keys, values)]
    )
    groups = [
        [2 * z + (z // NEAR + first) % 2 for z in range(chip, size, NEAR)]
        for chip in range(NEAR)
        for first in range(2)
    ]
    kv = lax.all_gather(kv, ("inner", "head"), axis_index_groups=groups, tiled=True)
    mine = jnp.concatenate([*payloads, kv])
    theirs = move(mine, swap)

    order = span_order[0]
    where = jnp.stack([place, core]).astype(jnp.int32)
    dq, parts, first = None, [], 0
    for count in CALLS:
        dq, part = attention_grads(first, count, heads, toks, order, where, mine, theirs, dq)
        parts += [part[i : i + BUNDLE] for i in range(0, count, BUNDLE)]
        first += count

    def role_of(z, c):
        return (c + z // NEAR // BUNDLE) % 2

    def hop(blocks):
        def target(z, c):
            role = role_of(z, c)
            z = (z + (blocks if role else -blocks) * NEAR) % size
            return z, role_of(z, role)

        return target

    def last_one(z, c):
        after = (z + NEAR) % size
        return (after, role_of(after, 0)) if role_of(z, c) else (z, 1 - c)

    def last_two(z, c):
        return hop(1)(z, c) if role_of(z, c) else None

    total = parts[0].astype(jnp.bfloat16)
    for part in parts[1:]:
        total = move(total, hop(BUNDLE))
        sums = total.astype(jnp.float32) + part
        total = sums.astype(jnp.bfloat16)
    total = move(total[0], hop(1)).astype(jnp.float32) + sums[1]
    total = total.astype(jnp.bfloat16)
    one = move(total, last_one)
    two = move(total, last_two)
    two = jnp.where(role_of(place, core) == 0, total, two)
    dkv = (one.astype(jnp.float32) + two.astype(jnp.float32)).astype(jnp.bfloat16)

    dq_theirs = move(dq[NEAR:].astype(jnp.bfloat16), swap)
    dq_mine = dq[:NEAR] + dq_theirs.astype(jnp.float32)
    dq_back = [dq_mine[i].astype(jnp.bfloat16) for i in range(1, NEAR)]
    backs = [move(dq_back[i - 1], near(i)) for i in range(1, NEAR)]
    query_grad = dq_mine[0] + sum(back.astype(jnp.float32) for back in backs)
    query_grad = query_grad.astype(jnp.bfloat16).reshape(heads, toks, width)
    query_grad = jnp.transpose(query_grad, (1, 0, 2))
    return query_grad[None], dkv[None, :, :width], dkv[None, :, width:]


def solution(mesh):
    in_specs = (
        P(("groups", "outer"), "inner", "head", None),
        P(("groups", "outer"), "inner", None),
        P(("groups", "outer"), "inner", None),
        P(("groups", "outer"), "inner", "head", None),
        P(("groups", "outer"), "head", "inner"),
        P(("groups", "outer"), "inner", "head", None),
        P(("groups", "outer"), None),
    )
    out_specs = (
        P(("groups", "outer"), "inner", "head", None),
        P(("groups", "outer"), "inner", None),
        P(("groups", "outer"), "inner", None),
    )
    return jax.shard_map(body, mesh=mesh, in_specs=in_specs, out_specs=out_specs, check_vma=False)
```

```python
import functools
import math

import jax
import jax.numpy as jnp
from jax import lax
from jax.experimental import pallas as pl
from jax.experimental.pallas import tpu as pltpu
from jax.sharding import PartitionSpec as P


LOG2E = math.log2(math.e)
NEAR = 2
BUNDLE = 2
CALLS = (2, 4, 2)
STAT_ROWS = 16


def rows_kernel(where, *refs):
    sources, (payload, kv), held, sems = refs[:6], refs[6:8], refs[8:12], refs[12]
    half = kv.shape[0] // 2
    start = pl.multiple_of(where[1] * half, half)
    sources = [*sources[:4], *[source.at[pl.ds(start, half)] for source in sources[4:]]]
    held = [*held, kv.at[pl.ds(0, half)], kv.at[pl.ds(half, half)]]
    copies = [
        pltpu.make_async_copy(source, target, sems.at[i])
        for i, (source, target) in enumerate(zip(sources, held))
    ]
    for copy in copies:
        copy.start()
    for copy in copies:
        copy.wait()
    queries, d_out, out, log_total = held[:4]
    toks, heads, width = queries.shape
    rows = heads * toks
    deltas = []
    for h in range(heads):
        grad = d_out[:, h, :]
        payload[h * toks : (h + 1) * toks] = queries[:, h, :]
        payload[rows + h * toks : rows + (h + 1) * toks] = grad
        product = out[:, h, :].astype(jnp.float32) * grad.astype(jnp.float32)
        deltas.append(jnp.sum(product.T, axis=0, keepdims=True))
    rest = jnp.concatenate([log_total[...] * LOG2E, *deltas])
    rest = jnp.concatenate([rest, jnp.zeros((STAT_ROWS - 2 * heads, width), jnp.float32)])
    for i in range(3):
        term = rest.astype(jnp.bfloat16)
        payload[2 * rows + i * STAT_ROWS : 2 * rows + (i + 1) * STAT_ROWS] = term
        rest = rest - term.astype(jnp.float32)


def own_rows(where, *arrays):
    toks, heads, width = arrays[0].shape
    return pl.pallas_call(
        rows_kernel,
        out_shape=(
            jax.ShapeDtypeStruct((2 * heads * toks + 3 * STAT_ROWS, width), jnp.bfloat16),
            jax.ShapeDtypeStruct((toks, width), jnp.bfloat16),
        ),
        in_specs=[pl.BlockSpec(memory_space=pltpu.SMEM)]
        + [pl.BlockSpec(memory_space=pltpu.HBM)] * len(arrays),
        out_specs=(pl.BlockSpec(memory_space=pltpu.VMEM),) * 2,
        scratch_shapes=[pltpu.VMEM(a.shape, a.dtype) for a in arrays[:4]]
        + [pltpu.SemaphoreType.DMA((len(arrays),))],
        compiler_params=pltpu.CompilerParams(vmem_limit_bytes=63 * 1024 * 1024),
        cost_estimate=pl.CostEstimate(
            flops=4 * heads * toks * width,
            bytes_accessed=10 * heads * toks * width,
            transcendentals=0,
        ),
    )(where, *arrays)


def kernel(first, count, heads, toks, order, where, mine, theirs, *refs):
    fresh = first == 0
    dq, dkv = refs if fresh else refs[1:]
    rows = heads * toks
    payload = 2 * rows + 3 * STAT_ROWS
    span_rows = toks // 2
    width = mine.shape[1]
    keys = NEAR * payload
    ring = (mine.shape[0] - keys) // toks
    scale = 1.0 / math.sqrt(width)
    place, core = where[0], where[1]
    step, member = place // NEAR, place % NEAR
    role = lax.rem(core + step // BUNDLE, 2)
    token = lax.broadcasted_iota(jnp.int32, (toks, toks), 1)
    row = lax.broadcasted_iota(jnp.int32, (toks, toks), 0)
    key_row, token_row = row % span_rows, token % span_rows
    nt = (((1,), (1,)), ((), ()))
    tn = (((0,), (0,)), ((), ()))

    def one_bundle(index):
        ks, vs, positions = [], [], []
        for j in range(BUNDLE):
            turn = first + index * BUNDLE + j
            ahead = jnp.where(role == 0, turn - (ring // 2 - 1), ring // 2 - turn)
            block = lax.rem(step + ahead + ring, ring)
            chip = block * NEAR + member
            start = pl.multiple_of(keys + block * toks, STAT_ROWS)
            a, b = mine[pl.ds(start, toks)], theirs[pl.ds(start, toks)]
            first_span = lax.rem(block + step + core, 2) == 0
            low, high = jnp.where(first_span, a, b), jnp.where(first_span, b, a)
            ks += [low[:span_rows], high[:span_rows]]
            vs += [low[span_rows:], high[span_rows:]]
            key_span = jnp.where(row < span_rows, order[2 * chip], order[2 * chip + 1])
            positions.append(key_span * span_rows + key_row)
        k, v, key_pos = jnp.concatenate(ks), jnp.concatenate(vs), jnp.concatenate(positions)
        dk = jnp.zeros((BUNDLE * toks, width), jnp.float32)
        dv = jnp.zeros((BUNDLE * toks, width), jnp.float32)
        for near in range(NEAR):
            near_chip = step * NEAR + (member ^ near)
            span = jnp.where(token < span_rows, order[2 * near_chip], order[2 * near_chip + 1])
            query_pos = span * span_rows + token_row
            visible = key_pos <= jnp.concatenate([query_pos] * BUNDLE)
            base = near * payload
            for part, source in ((near, mine), (NEAR + near, theirs)):
                q = source[base : base + rows]
                d = source[base + rows : base + 2 * rows]
                stat = [
                    source[base + 2 * rows + i * STAT_ROWS : base + 2 * rows + (i + 1) * STAT_ROWS]
                    for i in range(3)
                ]
                stat = sum(x.astype(jnp.float32) for x in stat)
                s = lax.dot_general(k, q, nt, preferred_element_type=jnp.float32)
                g = lax.dot_general(v, d, nt, preferred_element_type=jnp.float32)
                probs, grads = [], []
                for h in range(heads):
                    cols = slice(h * toks, (h + 1) * toks)
                    p = jnp.exp2(s[:, cols] * (scale * LOG2E) - stat[h : h + 1])
                    p = jnp.where(visible, p, 0.0)
                    probs.append(p.astype(jnp.bfloat16))
                    ds = p * (g[:, cols] - stat[heads + h : heads + h + 1]) * scale
                    grads.append(ds.astype(jnp.bfloat16))
                p = jnp.concatenate(probs, axis=1)
                ds = jnp.concatenate(grads, axis=1)
                dv = dv + jnp.dot(p, d, preferred_element_type=jnp.float32)
                dk = dk + jnp.dot(ds, q, preferred_element_type=jnp.float32)
                dq_part = lax.dot_general(ds, k, tn, preferred_element_type=jnp.float32)
                if index > 0:
                    dq_part += dq[part]
                elif not fresh:
                    dq_part += refs[0][part]
                dq[part] = dq_part
        for j in range(BUNDLE):
            dkv[index * BUNDLE + j, :, :width] = dk[j * toks : (j + 1) * toks]
            dkv[index * BUNDLE + j, :, width:] = dv[j * toks : (j + 1) * toks]

    for index in range(count // BUNDLE):
        one_bundle(index)


def attention_grads(first, count, heads, toks, order, where, mine, theirs, dq):
    width = mine.shape[1]
    rows = heads * toks
    smem = pl.BlockSpec(memory_space=pltpu.SMEM)
    vmem = pl.BlockSpec(memory_space=pltpu.VMEM)
    operands = [order, where, mine, theirs] + ([] if dq is None else [dq])
    return pl.pallas_call(
        functools.partial(kernel, first, count, heads, toks),
        out_shape=(
            jax.ShapeDtypeStruct((2 * NEAR, rows, width), jnp.float32),
            jax.ShapeDtypeStruct((count, toks, 2 * width), jnp.float32),
        ),
        in_specs=[smem, smem] + [vmem] * (len(operands) - 2),
        out_specs=(vmem, vmem),
        input_output_aliases={} if dq is None else {len(operands) - 1: 0},
        compiler_params=pltpu.CompilerParams(vmem_limit_bytes=16 * 1024 * 1024),
        cost_estimate=pl.CostEstimate(
            flops=2 * 5 * 2 * NEAR * rows * count * toks * width,
            bytes_accessed=8 * rows * width * 4,
            transcendentals=2 * NEAR * rows * count * toks,
        ),
    )(*operands)


def body(queries, keys, values, out, log_total, d_out, span_order):
    size = lax.axis_size("inner")
    place = lax.axis_index("inner")
    core = lax.axis_index("head")
    toks, heads, width = queries.shape[1:]

    def move(array, target):
        pairs = []
        for z in range(size):
            for c in range(2):
                to = target(z, c)
                if to is not None:
                    pairs.append((2 * z + c, 2 * (to[0] % size) + to[1]))
        return lax.ppermute(array, ("inner", "head"), pairs)

    def swap(z, c):
        return z, 1 - c

    def near(distance):
        return lambda z, c: (z ^ distance, c)

    where = jnp.stack([place, core]).astype(jnp.int32)
    payload, kv = own_rows(
        where, queries[0], d_out[0], out[0], log_total[0], keys[0], values[0]
    )
    payloads = [payload] + [move(payload, near(i)) for i in range(1, NEAR)]

    groups = [
        [2 * z + (z // NEAR + first) % 2 for z in range(chip, size, NEAR)]
        for chip in range(NEAR)
        for first in range(2)
    ]
    kv = lax.all_gather(kv, ("inner", "head"), axis_index_groups=groups, tiled=True)
    mine = jnp.concatenate([*payloads, kv])
    theirs = move(mine, swap)

    order = span_order[0]
    dq, parts, first = None, [], 0
    for count in CALLS:
        dq, part = attention_grads(first, count, heads, toks, order, where, mine, theirs, dq)
        parts += [part[i : i + BUNDLE] for i in range(0, count, BUNDLE)]
        first += count

    def role_of(z, c):
        return (c + z // NEAR // BUNDLE) % 2

    def hop(blocks):
        def target(z, c):
            role = role_of(z, c)
            z = (z + (blocks if role else -blocks) * NEAR) % size
            return z, role_of(z, role)

        return target

    def last_one(z, c):
        after = (z + NEAR) % size
        return (after, role_of(after, 0)) if role_of(z, c) else (z, 1 - c)

    def last_two(z, c):
        return hop(1)(z, c) if role_of(z, c) else None

    total = parts[0].astype(jnp.bfloat16)
    for part in parts[1:]:
        total = move(total, hop(BUNDLE))
        sums = total.astype(jnp.float32) + part
        total = sums.astype(jnp.bfloat16)
    total = move(total[0], hop(1)).astype(jnp.float32) + sums[1]
    total = total.astype(jnp.bfloat16)
    one = move(total, last_one)
    two = move(total, last_two)
    two = jnp.where(role_of(place, core) == 0, total, two)
    dkv = (one.astype(jnp.float32) + two.astype(jnp.float32)).astype(jnp.bfloat16)

    dq_theirs = move(dq[NEAR:].astype(jnp.bfloat16), swap)
    dq_mine = dq[:NEAR] + dq_theirs.astype(jnp.float32)
    dq_back = [dq_mine[i].astype(jnp.bfloat16) for i in range(1, NEAR)]
    backs = [move(dq_back[i - 1], near(i)) for i in range(1, NEAR)]
    query_grad = dq_mine[0] + sum(back.astype(jnp.float32) for back in backs)
    query_grad = query_grad.astype(jnp.bfloat16).reshape(heads, toks, width)
    query_grad = jnp.transpose(query_grad, (1, 0, 2))
    return query_grad[None], dkv[None, :, :width], dkv[None, :, width:]


def solution(mesh):
    in_specs = (
        P(("groups", "outer"), "inner", "head", None),
        P(("groups", "outer"), "inner", None),
        P(("groups", "outer"), "inner", None),
        P(("groups", "outer"), "inner", "head", None),
        P(("groups", "outer"), "head", "inner"),
        P(("groups", "outer"), "inner", "head", None),
        P(("groups", "outer"), None),
    )
    out_specs = (
        P(("groups", "outer"), "inner", "head", None),
        P(("groups", "outer"), "inner", None),
        P(("groups", "outer"), "inner", None),
    )
    return jax.shard_map(body, mesh=mesh, in_specs=in_specs, out_specs=out_specs, check_vma=False)
```
